16 devices in a mesh: sweep: 2 (over z), ent: 8 (over y, x, core).
Axes of the slice: x: 2, y: 2, z: 2, core: 2. Of those that a mesh axis runs over, the one named last changes fastest.
Arguments:
- ent_table: float32 [262144, 400], P(('sweep', 'ent')), parts along dimension 0
- ada_state: float32 [262144], P(('sweep', 'ent')), parts along dimension 0
- rel_table: float32 [2690, 400], P('sweep'), parts along dimension 0
- head_idx: int32 [16, 6, 1024], P(('sweep', 'ent')), parts along dimension 0
- tail_idx: int32 [16, 6, 1024], P(('sweep', 'ent')), parts along dimension 0
- rel_idx: int32 [16, 6, 1024], P(('sweep', 'ent')), parts along dimension 0
- neg_idx: int32 [16, 6, 1024], P(('sweep', 'ent')), parts along dimension 0
- edge_mask: int32 [16, 6, 1024], P(('sweep', 'ent')), parts along dimension 0
Outputs:
- output 1: float32 [262144, 400], P(('sweep', 'ent')), parts along dimension 0
- output 2: float32 [262144], P(('sweep', 'ent')), parts along dimension 0
- output 3: float32 [2690, 400], P('sweep'), parts along dimension 0
- output 4: float32 [16, 6], P(('sweep', 'ent')), parts along dimension 0
There are 2 independent parts. The reference program is written for one: setup_inputs(seed, part) draws one part's arguments, and reference() takes and returns one part's arrays. A program takes and returns all parts, laid end to end along the dimension named above; each array names one.
All inputs are finite; a program needn't handle non-finite values.
Results may differ from the reference program's by a relative error of at most 0.00243552.
Values are sent between devices in bfloat16 or wider.
A program may use at most 1 GiB of HBM per device.

```python
import jax
import jax.numpy as jnp
from jax import lax

EMB_DIM = 400
REL_COUNT = 1345
NEG_COUNT = 1024
EDGE_COUNT = 1024
PART_ROWS = 16384
ROUNDS = 6
ENT_DEVS = 8

LEARN_RATE = 0.25
ADA_EPS = 1e-10
HOT_ROWS = PART_ROWS // 32
HOT_RELS = (REL_COUNT + 7) // 8


def draw_rows(key, shape, limit, hot_count):
    key_pick, key_wide, key_hot = jax.random.split(key, 3)
    hot_pick = jax.random.randint(key_pick, shape, 0, 2)
    wide_ids = jax.random.randint(key_wide, shape, 0, limit)
    hot_ids = jax.random.randint(key_hot, shape, 0, hot_count)
    picked = jnp.where(hot_pick == 1, hot_ids, wide_ids)
    return picked.at[0, 0, 0].set(limit - 1).astype(jnp.int32)


def setup_inputs(seed: int = 0, part: int = 0) -> dict:
    base_key = jax.random.key(seed)
    part_key = jax.random.fold_in(base_key, part)
    key_list = jax.random.split(part_key, 9)
    total_rows = ENT_DEVS * PART_ROWS
    edge_shape = (ENT_DEVS, ROUNDS, EDGE_COUNT)
    ent_table = jax.random.normal(key_list[0], (total_rows, EMB_DIM), jnp.float32)
    ada_state = jnp.exp2(-12.0 * jax.random.uniform(key_list[1], (total_rows,), jnp.float32)) / EMB_DIM
    rel_table = jax.random.normal(key_list[2], (REL_COUNT, EMB_DIM), jnp.float32) * (0.5 ** 0.5)
    head_idx = draw_rows(key_list[3], edge_shape, PART_ROWS, HOT_ROWS)
    tail_idx = draw_rows(key_list[4], edge_shape, PART_ROWS, HOT_ROWS)
    rel_idx = draw_rows(key_list[5], edge_shape, REL_COUNT, HOT_RELS)
    neg_idx = draw_rows(key_list[6], (ENT_DEVS, ROUNDS, NEG_COUNT), PART_ROWS, HOT_ROWS)
    fill_count = jax.random.randint(key_list[7], (ENT_DEVS, ROUNDS, 1), 0, EDGE_COUNT + 1)
    edge_mask = (jax.random.randint(key_list[8], edge_shape, 0, EDGE_COUNT) < fill_count).astype(jnp.int32)
    return {'ent_table': ent_table, 'ada_state': ada_state, 'rel_table': rel_table, 'head_idx': head_idx, 'tail_idx': tail_idx, 'rel_idx': rel_idx, 'neg_idx': neg_idx, 'edge_mask': edge_mask}


def bucket_grads(head_rows, tail_bf, neg_bf, rel_rows, weight):
    half_dim = EMB_DIM // 2
    score_scale = EMB_DIM ** -0.5
    h_re = head_rows[:, :half_dim]
    h_im = head_rows[:, half_dim:]
    r_re = rel_rows[:, :half_dim]
    r_im = rel_rows[:, half_dim:]
    query = jnp.concatenate([h_re * r_re - h_im * r_im, h_re * r_im + h_im * r_re], axis=1)
    query_bf = query.astype(jnp.bfloat16)
    tail_rows = tail_bf.astype(jnp.float32)
    pos_score = score_scale * jnp.sum(query * tail_rows, axis=1)
    neg_score = score_scale * jnp.dot(query_bf, neg_bf.T, preferred_element_type=jnp.float32)
    top_score = jnp.maximum(pos_score, jnp.max(neg_score, axis=1))
    pos_exp = jnp.exp(pos_score - top_score)
    neg_exp = jnp.exp(neg_score - top_score[:, None])
    denom_sum = pos_exp + jnp.sum(neg_exp, axis=1)
    weight_f = weight.astype(jnp.float32)
    loss_sum = jnp.sum(weight_f * (top_score + jnp.log(denom_sum) - pos_score))
    d_pos = weight_f * (pos_exp / denom_sum - 1.0)
    d_negs = ((weight_f / denom_sum)[:, None] * neg_exp).astype(jnp.bfloat16)
    d_query = score_scale * (d_pos[:, None] * tail_rows + jnp.dot(d_negs, neg_bf, preferred_element_type=jnp.float32))
    d_tail = score_scale * d_pos[:, None] * query
    d_neg = score_scale * jnp.dot(d_negs.T, query_bf, preferred_element_type=jnp.float32)
    dq_re = d_query[:, :half_dim]
    dq_im = d_query[:, half_dim:]
    d_head = jnp.concatenate([dq_re * r_re + dq_im * r_im, dq_im * r_re - dq_re * r_im], axis=1)
    d_rel = jnp.concatenate([dq_re * h_re + dq_im * h_im, dq_im * h_re - dq_re * h_im], axis=1)
    return loss_sum, d_head, d_tail, d_neg, d_rel


def adagrad_rows(table, state, row_grad):
    new_state = state + jnp.mean(row_grad * row_grad, axis=1)
    new_table = table - LEARN_RATE * row_grad / jnp.sqrt(new_state + ADA_EPS)[:, None]
    return new_table, new_state


def reference(ent_table, ada_state, rel_table, head_idx, tail_idx, rel_idx, neg_idx, edge_mask):
    dev_ids = jnp.arange(ENT_DEVS)
    head_base = dev_ids * PART_ROWS

    def round_body(carry, round_in):
        ent_cur, ada_cur, rel_cur, rel_acc = carry
        step, head_ids, tail_ids, rel_ids, neg_ids, mask_rows = round_in
        tail_base = ((dev_ids + step + 1) % ENT_DEVS) * PART_ROWS

        def one_bucket(bucket_in):
            head_off, tail_off, head_pick, tail_pick, rel_pick, neg_pick, mask_pick = bucket_in
            return bucket_grads(ent_cur[head_off + head_pick], ent_cur[tail_off + tail_pick].astype(jnp.bfloat16), ent_cur[tail_off + neg_pick].astype(jnp.bfloat16), rel_cur[rel_pick], mask_pick)

        loss_vals, d_head, d_tail, d_neg, d_rel = lax.map(one_bucket, (head_base, tail_base, head_ids, tail_ids, rel_ids, neg_ids, mask_rows))
        row_ids = jnp.concatenate([(head_base[:, None] + head_ids).reshape(-1), (tail_base[:, None] + tail_ids).reshape(-1), (tail_base[:, None] + neg_ids).reshape(-1)])
        row_grads = jnp.concatenate([d_head.reshape(-1, EMB_DIM), d_tail.reshape(-1, EMB_DIM), d_neg.reshape(-1, EMB_DIM)])
        row_grad = jax.ops.segment_sum(row_grads, row_ids, num_segments=ENT_DEVS * PART_ROWS)
        rel_grad = jax.ops.segment_sum(d_rel.reshape(-1, EMB_DIM), rel_ids.reshape(-1), num_segments=REL_COUNT)
        ent_cur, ada_cur = adagrad_rows(ent_cur, ada_cur, row_grad)
        rel_cur, rel_acc = adagrad_rows(rel_cur, rel_acc, rel_grad)
        return (ent_cur, ada_cur, rel_cur, rel_acc), loss_vals / EDGE_COUNT

    rel_zero = jnp.zeros((REL_COUNT,), jnp.float32)
    round_ins = (jnp.arange(ROUNDS), head_idx.transpose(1, 0, 2), tail_idx.transpose(1, 0, 2), rel_idx.transpose(1, 0, 2), neg_idx.transpose(1, 0, 2), edge_mask.transpose(1, 0, 2))
    final_state, loss_rounds = lax.scan(round_body, (ent_table, ada_state, rel_table, rel_zero), round_ins)
    return final_state[0], final_state[1], final_state[2], loss_rounds.T
```

```python
import functools

import jax
import jax.numpy as jnp
from jax import lax
from jax.experimental import pallas as pl
from jax.experimental.pallas import tpu as pltpu
from jax.sharding import PartitionSpec as P


LEARN_RATE = 0.25
ADA_EPS = 1e-10

DIM = 400
HALF = 200
ACC_LANE = 16
LANES = 128
MIB = 1 << 20
GRANT = 7

VM = pl.BlockSpec(memory_space=pltpu.VMEM)
SM = pl.BlockSpec(memory_space=pltpu.SMEM)
ANY = pl.BlockSpec(memory_space=pl.ANY)
F32 = jnp.float32
BF16 = jnp.bfloat16


def params(mib):
    return pltpu.CompilerParams(vmem_limit_bytes=mib * MIB)


def lane_ids(shape):
    return lax.broadcasted_iota(jnp.int32, shape, 1)


def swap_two(x):
    return pltpu.roll(x, 64, 1)


def swap_three(x):
    return jnp.where(lane_ids(x.shape) < 8, pltpu.roll(x, 120, 1), pltpu.roll(x, 8, 1))


def times(a, b):
    out = [a[0] * b[0] - a[1] * b[1], a[0] * b[1] + a[1] * b[0]]
    for x, y, swap, edge in ((a[2], b[2], swap_two, 64), (a[3], b[3], swap_three, 8)):
        xs, ys = swap(x), swap(y)
        out.append(jnp.where(lane_ids(x.shape) < edge, x * y - xs * ys, xs * y + x * ys))
    return out


def times_conj(a, b):
    out = [a[0] * b[0] + a[1] * b[1], a[1] * b[0] - a[0] * b[1]]
    for x, y, swap, edge in ((a[2], b[2], swap_two, 64), (a[3], b[3], swap_three, 8)):
        xs, ys = swap(x), swap(y)
        out.append(jnp.where(lane_ids(x.shape) < edge, x * y + xs * ys, x * ys - xs * y))
    return out


def keep_data(x):
    return jnp.where(lane_ids(x.shape) < ACC_LANE, x, 0.0)


def flat(ref):
    return ref.reshape(ref.shape[0] * 4, LANES)


def plane(ref2, start, rows, part):
    return ref2[pl.ds(start * 4 + part, rows, stride=4), :]


def put_plane(ref2, start, rows, part, x):
    ref2[pl.ds(start * 4 + part, rows, stride=4), :] = x


def copy_rows(idx_ref, count, src, dst, offset):
    def body(i, carry):
        dst[offset + i] = src[idx_ref[i]]
        return carry
    lax.fori_loop(0, count, body, 0, unroll=16)


def pack_rows(dst, src2, rows, first, groups, packed):
    step = rows // 8
    for g in range(groups):
        at, to = g * step, (first + g) * step
        for part in range(3):
            dst[part * rows + to:part * rows + to + step, :] = plane(src2, at, step, part).astype(dst.dtype)
        last = keep_data(plane(src2, at, step, 3))
        if first + g:
            last = pltpu.roll(last, 16 * (first + g), 1)
        packed = last if packed is None else packed + last
    if first + groups == 8:
        dst[3 * rows:3 * rows + step, :] = packed.astype(dst.dtype)
    return packed


def unpack_part(src, rows, g, step):
    planes = [src[part * rows + g * step:part * rows + (g + 1) * step, :].astype(F32) for part in range(3)]
    last = src[3 * rows:3 * rows + step, :].astype(F32)
    if g:
        last = pltpu.roll(last, LANES - 16 * g, 1)
    planes.append(keep_data(last))
    return planes


def load_kernel(head_ref, tail_ref, neg_ref, ent_ref, ada_ref, rel_ref, tab_ref, head_out, tail_out, hold_ref, *, areas):
    cols = ent_ref.shape[1]
    tab2 = flat(tab_ref)
    start = pl.program_id(0) * (cols * 4)
    parts = [
        ent_ref[0:128, :],
        ent_ref[HALF:HALF + 128, :],
        jnp.concatenate([ent_ref[128:192, :], ent_ref[HALF + 128:HALF + 192, :]], axis=0),
        jnp.concatenate([ent_ref[192:200, :], ent_ref[HALF + 192:HALF + 200, :], jnp.broadcast_to(ada_ref[...], (8, cols)), jnp.zeros((104, cols), F32)], axis=0),
    ]
    for part in range(4):
        x = parts[part].T
        if part == 3:
            x = jnp.where(lane_ids(x.shape) <= ACC_LANE, x, 0.0)
        tab2[pl.ds(start + part, cols, stride=4), :] = x

    @pl.when(pl.program_id(0) == pl.num_programs(0) - 1)
    def _():
        pltpu.sync_copy(rel_ref, tab_ref.at[pl.ds(*areas['rel'])])
        gather_rows(head_ref, tail_ref, neg_ref, tab_ref, hold_ref, head_out, tail_out)


def store_kernel(tab_ref, ent_ref, ada_ref, rel_ref, *, areas):
    cols = ent_ref.shape[1]
    tab2 = flat(tab_ref)
    start = pl.program_id(0) * (cols * 4)
    for part in range(4):
        x = tab2[pl.ds(start + part, cols, stride=4), :].T
        if part < 2:
            ent_ref[part * HALF:part * HALF + 128, :] = x
        elif part == 2:
            ent_ref[128:192, :] = x[0:64]
            ent_ref[HALF + 128:HALF + 192, :] = x[64:128]
        else:
            ent_ref[192:200, :] = x[0:8]
            ent_ref[HALF + 192:HALF + 200, :] = x[8:16]
            ada_ref[...] = x[ACC_LANE:ACC_LANE + 1]

    @pl.when(pl.program_id(0) == 0)
    def _():
        pltpu.sync_copy(tab_ref.at[pl.ds(*areas['rel'])], rel_ref)


def gather_rows(head_ref, tail_ref, neg_ref, tab_ref, hold_ref, head_out, tail_out):
    edges = head_ref.shape[0]
    hold2 = flat(hold_ref)
    copy_rows(tail_ref, edges, tab_ref, hold_ref, 0)
    packed = pack_rows(tail_out, hold2, 2 * edges, 0, 4, None)
    copy_rows(neg_ref, edges, tab_ref, hold_ref, 0)
    pack_rows(tail_out, hold2, 2 * edges, 4, 4, packed)
    copy_rows(head_ref, edges, tab_ref, hold_ref, 0)
    pack_rows(head_out, hold2, edges, 0, 8, None)


def adagrad(grad, row):
    total = grad[0] * grad[0] + grad[1] * grad[1] + grad[2] * grad[2] + grad[3] * grad[3]
    mean = jnp.sum(total, axis=1, keepdims=True) * (1.0 / DIM)
    lane = lane_ids(row[3].shape)
    state = jnp.sum(jnp.where(lane == ACC_LANE, row[3], 0.0), axis=1, keepdims=True) + mean
    rate = LEARN_RATE / jnp.sqrt(state + ADA_EPS)
    new = [row[part] - grad[part] * rate for part in range(4)]
    new[3] = jnp.where(lane == ACC_LANE, state, new[3])
    return new


def apply_rows(key_ref, grad_ref, tab_ref, sum_ref, row_ref):
    size = sum_ref.shape[0]
    sum2, row2 = flat(sum_ref), flat(row_ref)
    block = 128

    def chunk(c, carry):
        base = c * size

        def collect(e, carry):
            prev, acc, old = carry
            key = key_ref[base + e]
            row = key >> 12
            same = row == prev
            g = grad_ref[key & 4095]
            acc = jnp.where(same, acc + g, g)
            old = jnp.where(same, old, tab_ref[row])
            sum_ref[e] = acc
            row_ref[e] = old
            return row, acc, old

        carry = lax.fori_loop(0, size, collect, carry, unroll=16)

        def update(b, carry):
            at = b * (block * 4)
            grad = [sum2[pl.ds(at + part, block, stride=4), :] for part in range(4)]
            row = [row2[pl.ds(at + part, block, stride=4), :] for part in range(4)]
            new = adagrad(grad, row)
            for part in range(4):
                row2[pl.ds(at + part, block, stride=4), :] = new[part]
            return carry

        lax.fori_loop(0, size // block, update, 0)

        def write(e, carry):
            tab_ref[key_ref[base + e] >> 12] = row_ref[e]
            return carry

        lax.fori_loop(0, size, write, 0, unroll=16)
        return carry

    zero = jnp.zeros((4, LANES), F32)
    lax.fori_loop(0, key_ref.shape[0] // size, chunk, (jnp.int32(-1), zero, zero))


def update_kernel(key_ref, head_ref, tail_ref, neg_ref, head_out, tail_out, tab_ref, sum_ref, row_ref, *, areas):
    apply_rows(key_ref, tab_ref.at[pl.ds(*areas['grad'])], tab_ref, sum_ref, row_ref)
    gather_rows(head_ref, tail_ref, neg_ref, tab_ref, sum_ref, head_out, tail_out)


def last_kernel(key_ref, tab_ref, sum_ref, row_ref, *, areas):
    apply_rows(key_ref, tab_ref.at[pl.ds(*areas['grad'])], tab_ref, sum_ref, row_ref)


def put_wide(ref, start, rows, planes):
    for part in range(4):
        ref[start:start + rows, part * LANES:(part + 1) * LANES] = planes[part].astype(ref.dtype)


def make_query(rel_ref, rel_tab, head_ref, tail_ref, hold_ref, query_ref, neg_ref):
    edges = rel_ref.shape[0]
    copy_rows(rel_ref, edges, rel_tab, hold_ref, 0)
    hold2 = flat(hold_ref)
    step = edges // 8
    wide = 2 * step
    for g in range(4):
        put_wide(neg_ref, g * wide, wide, unpack_part(tail_ref, 2 * edges, g + 4, wide))
    for g in range(8):
        heads = unpack_part(head_ref, edges, g, step)
        rels = [plane(hold2, g * step, step, part) for part in range(4)]
        rels[3] = keep_data(rels[3])
        put_wide(query_ref, g * step, step, times(heads, rels))
    return DIM ** -0.5


def tail_block(tail_ref, b, block):
    rows = 8 * block
    planes = [tail_ref[pl.ds(pl.multiple_of(part * rows + b * block, block), block), :].astype(F32) for part in range(3)]
    last = tail_ref[3 * rows:3 * rows + block, :].astype(F32)
    planes.append(keep_data(pltpu.roll(last, LANES - 16 * b, 1)))
    return planes


def head_kernel(rel_ref, key_ref, weight_ref, head_ref, tail_ref, give_out, loss_out, tab_ref, query_ref, neg_ref, *, areas, step_no):
    rel_tab, grad_out = tab_ref.at[pl.ds(*areas['rel'])], tab_ref.at[pl.ds(*areas['grad'])]
    edges = rel_ref.shape[0]
    hold_ref = grad_out.at[pl.ds(edges, edges)]
    scale = make_query(rel_ref, rel_tab, head_ref, tail_ref, hold_ref, query_ref, neg_ref)
    block = edges // 4

    def body(b, loss):
        at = pl.ds(pl.multiple_of(b * block, block), block)
        query = query_ref[at, :]
        tails = jnp.concatenate(tail_block(tail_ref, b, block), axis=1)
        pos = scale * jnp.sum(query * tails, axis=1, keepdims=True)
        neg = scale * lax.dot_general(query.astype(BF16), neg_ref[...], (((1,), (1,)), ((), ())), preferred_element_type=F32)
        top = jnp.maximum(pos, jnp.max(neg, axis=1, keepdims=True))
        pos_exp = jnp.exp(pos - top)
        neg_exp = jnp.exp(neg - top)
        denom = pos_exp + jnp.sum(neg_exp, axis=1, keepdims=True)
        weight = weight_ref[at, step_no:step_no + 1]
        loss = loss + weight * (top + jnp.log(denom) - pos)
        d_pos = weight * (pos_exp / denom - 1.0)
        d_neg = ((weight / denom) * neg_exp).astype(BF16)
        query_ref[at, :] = scale * (d_pos * tails + jnp.dot(d_neg, neg_ref[...], preferred_element_type=F32))
        return loss

    loss = lax.fori_loop(0, edges // block, body, jnp.zeros((block, 1), F32))
    loss_out[0] = jnp.sum(loss)
    hold2, grad2 = flat(hold_ref), flat(grad_out)
    step = edges // 8
    for g in range(8):
        at = g * step
        heads = unpack_part(head_ref, edges, g, step)
        rels = [plane(hold2, at, step, part) for part in range(4)]
        rels[3] = keep_data(rels[3])
        d_query = [query_ref[at:at + step, part * LANES:(part + 1) * LANES] for part in range(4)]
        d_head = times_conj(d_query, rels)
        d_rel = times_conj(d_query, heads)
        for part in range(4):
            put_plane(grad2, at, step, part, d_head[part])
            put_plane(hold2, at, step, part, d_rel[part])

    rel_rows = rel_tab.shape[0]
    sum_ref = grad_out.at[pl.ds(2 * edges, rel_rows)]
    sum_ref[...] = jnp.zeros(sum_ref.shape, F32)

    def scatter(e, carry):
        prev, acc = carry
        key = key_ref[e]
        row = key >> 10
        g = hold_ref[key & 1023]
        acc = jnp.where(row == prev, acc + g, g)
        sum_ref[row] = acc
        return row, acc

    lax.fori_loop(0, edges, scatter, (jnp.int32(-1), jnp.zeros((4, LANES), F32)), unroll=16)
    drel_out = flat(tab_ref.at[pl.ds(*areas['drel'])])
    pack_rows(drel_out, flat(sum_ref), rel_rows, 0, 8, None)
    used, half = rel_rows * 25 // 8, give_out.shape[0]
    drel_out[used:, :] = jnp.zeros((2 * half - used, LANES), F32)
    core = lax.rem(lax.axis_index('ent'), 2)
    give_out[...] = drel_out[pl.ds(pl.multiple_of((1 - core) * half, 8), half), :]


def tail_kernel(rel_ref, weight_ref, head_ref, tail_ref, tab_ref, query_ref, neg_ref, sum_ref, *, areas):
    rel_tab, grad_out = tab_ref.at[pl.ds(*areas['rel'])], tab_ref.at[pl.ds(*areas['grad'])]
    edges = rel_ref.shape[0]
    hold_ref = grad_out.at[pl.ds(edges, edges)]
    scale = make_query(rel_ref, rel_tab, head_ref, tail_ref, hold_ref, query_ref, neg_ref)
    block = edges // 4
    grad2 = flat(grad_out)
    sum_ref[...] = jnp.zeros(sum_ref.shape, F32)

    def body(b, carry):
        at = pl.ds(pl.multiple_of(b * block, block), block)
        query = query_ref[at, :]
        query_bf = query.astype(BF16)
        tails = tail_block(tail_ref, b, block)
        prod = [query[:, part * LANES:(part + 1) * LANES] * tails[part] for part in range(4)]
        prod = (prod[0] + prod[1]) + (prod[2] + prod[3])
        pos = scale * jnp.sum(prod.T, axis=0, keepdims=True)
        neg = scale * lax.dot_general(neg_ref[...], query_bf, (((1,), (1,)), ((), ())), preferred_element_type=F32)
        top = jnp.maximum(pos, jnp.max(neg, axis=0, keepdims=True))
        pos_exp = jnp.exp(pos - top)
        neg_exp = jnp.exp(neg - top)
        denom = pos_exp + jnp.sum(neg_exp, axis=0, keepdims=True)
        weight = weight_ref[pl.ds(b, 1), :]
        d_pos = weight * (pos_exp / denom - 1.0)
        d_neg = ((weight / denom) * neg_exp).astype(BF16)
        sum_ref[...] += jnp.dot(d_neg, query_bf, preferred_element_type=F32)
        d_pos_col = jnp.broadcast_to(d_pos, (LANES, block)).T
        for part in range(4):
            grad2[pl.ds((edges + b * block) * 4 + part, block, stride=4), :] = scale * d_pos_col * query[:, part * LANES:(part + 1) * LANES]
        return carry

    lax.fori_loop(0, edges // block, body, 0)
    for part in range(4):
        put_plane(grad2, 2 * edges, edges, part, scale * sum_ref[:, part * LANES:(part + 1) * LANES])


def split_kernel(got_ref, own_out, one_out, two_out, three_out, tab_ref, *, areas):
    drel_ref = flat(tab_ref.at[pl.ds(*areas['drel'])])
    half, piece = got_ref.shape[0], own_out.shape[0]
    me = lax.axis_index('ent')
    core, chip = lax.rem(me, 2), lax.div(me, 2)
    for away, out in enumerate((own_out, one_out, two_out, three_out)):
        at = pl.multiple_of((chip ^ away) * piece, 8)
        out[...] = drel_ref[pl.ds(pl.multiple_of(core * half + at, 8), piece), :] + got_ref[pl.ds(at, piece), :]


def sum_kernel(own_ref, one_ref, two_ref, three_ref, out, tab_ref, *, areas):
    out[...] = (own_ref[...] + one_ref[...]) + (two_ref[...] + three_ref[...])


def join_kernel(own_ref, one_ref, two_ref, three_ref, out, tab_ref, *, areas):
    piece = own_ref.shape[0]
    chip = lax.div(lax.axis_index('ent'), 2)
    for away, ref in enumerate((own_ref, one_ref, two_ref, three_ref)):
        out[pl.ds(pl.multiple_of((chip ^ away) * piece, 8), piece), :] = ref[...]


def rel_kernel(half_ref, far_ref, tab_ref, *, areas):
    drel_ref = flat(tab_ref.at[pl.ds(*areas['drel'])])
    rel_tab = tab_ref.at[pl.ds(*areas['rel'])]
    rows = rel_tab.shape[0]
    half = half_ref.shape[0]
    core = lax.rem(lax.axis_index('ent'), 2)
    drel_ref[pl.ds(pl.multiple_of(core * half, 8), half), :] = half_ref[...]
    drel_ref[pl.ds(pl.multiple_of((1 - core) * half, 8), half), :] = far_ref[...]
    step = rows // 8
    rel2 = flat(rel_tab)
    for g in range(8):
        grad = unpack_part(drel_ref, rows, g, step)
        row = [plane(rel2, g * step, step, part) for part in range(4)]
        new = adagrad(grad, row)
        for part in range(4):
            put_plane(rel2, g * step, step, part, new[part])


def shape(*dims, dtype=F32):
    return jax.ShapeDtypeStruct(dims, dtype)


def split_rows(table, pad_rows):
    rows = table.shape[0]
    table = jnp.pad(table, ((0, pad_rows - rows), (0, 0)))
    re, im = table[:, :HALF], table[:, HALF:]
    last = jnp.concatenate([re[:, 192:], im[:, 192:], jnp.zeros((pad_rows, LANES - 16), F32)], axis=1)
    return jnp.stack([re[:, :128], im[:, :128], jnp.concatenate([re[:, 128:192], im[:, 128:192]], axis=1), last], axis=1)


def join_rows(table, rows):
    t = table[:rows]
    return jnp.concatenate([t[:, 0], t[:, 2, :64], t[:, 3, :8], t[:, 1], t[:, 2, 64:], t[:, 3, 8:16]], axis=1)


def solution(mesh):
    ent_devs = mesh.shape['ent']
    row_spec = P(('sweep', 'ent'), None)
    state_spec = P(('sweep', 'ent'))
    rel_spec = P('sweep', None)
    edge_spec = P(('sweep', 'ent'), None, None)

    def per_device(ent_part, ada_part, rel_table, head_idx, tail_idx, rel_idx, neg_idx, edge_mask):
        part_rows = ent_part.shape[0]
        rel_count = rel_table.shape[0]
        rounds = head_idx.shape[1]
        edges = head_idx.shape[2]
        rel_rows = -(-rel_count // 128) * 128
        head_idx, tail_idx, rel_idx, neg_idx, edge_mask = (x[0] for x in (head_idx, tail_idx, rel_idx, neg_idx, edge_mask))

        piece = -(-(rel_rows * 25 // 8) // 64) * 8

        def away(bits):
            return [(sender, sender ^ bits) for sender in range(ent_devs)]

        def ring(step):
            shift = step + 1
            to_owner = [(sender, (sender + shift) % ent_devs) for sender in range(ent_devs)]
            return to_owner, [(target, sender) for sender, target in to_owner]

        asked = jnp.stack([tail_idx, neg_idx, rel_idx, edge_mask], axis=1)
        served = jnp.stack([lax.ppermute(asked[step], 'ent', ring(step)[0]) for step in range(rounds)])
        rows_all = jnp.concatenate([head_idx, served[:, 0], served[:, 1]], axis=1)
        keys = lax.sort(rows_all * 4096 + jnp.arange(3 * edges, dtype=jnp.int32)[None, :], dimension=1, is_stable=False)
        rel_keys = lax.sort(rel_idx * 1024 + jnp.arange(edges, dtype=jnp.int32)[None, :], dimension=1, is_stable=False)
        own_weight = jnp.pad(edge_mask.astype(F32), ((0, 8 - rounds), (0, 0))).T
        serve_weight = served[:, 3].astype(F32).reshape(rounds, edges // 256, 256)
        rel_tab = split_rows(rel_table, rel_rows)
        small = []
        for step in range(rounds):
            small.append((head_idx[step], served[step, 0], served[step, 1], served[step, 2], rel_idx[step], keys[step], rel_keys[step], serve_weight[step]))
        small, own_weight, rel_tab, ent_cols, ada_row = lax.optimization_barrier((small, own_weight, rel_tab, ent_part.T, ada_part.reshape(1, part_rows)))

        cols = 512
        grad_rows = 2 * edges + max(edges, rel_rows)
        areas = {'grad': (part_rows, grad_rows), 'rel': (part_rows + grad_rows, rel_rows), 'drel': (part_rows + grad_rows + rel_rows, 2 * piece)}
        tab_shape = pltpu.VMEM((sum(areas['drel']), 4, LANES), F32)
        head_wire, tail_wire = shape(edges * 25 // 8, LANES), shape(2 * edges * 25 // 8, LANES, dtype=BF16)
        part_wire, half_wire = shape(piece, LANES), shape(4 * piece, LANES)
        hold = pltpu.VMEM((edges, 4, LANES), F32)
        work = [pltpu.VMEM((edges, 512), F32), pltpu.VMEM((edges, 512), BF16)]

        def call(kernel, name, tab, inputs, in_specs, out_shape, out_specs, scratch=(), **more):
            ins, outs = len(inputs), len(out_shape)

            def body(*refs):
                kernel(*refs[:ins], *refs[ins + 1:], areas=areas, **more)

            got = pl.pallas_call(
                body, in_specs=in_specs + [VM], out_specs=out_specs + [VM], out_shape=out_shape + [tab_shape],
                input_output_aliases={ins: outs}, scratch_shapes=list(scratch), compiler_params=params(GRANT), name=name)(*inputs, tab)
            return got[-1], got[:-1]

        tab, heads, tails = pl.pallas_call(
            functools.partial(load_kernel, areas=areas), grid=(part_rows // cols,),
            in_specs=[SM, SM, SM, pl.BlockSpec((DIM, cols), lambda i: (0, i)), pl.BlockSpec((1, cols), lambda i: (0, i)), ANY],
            out_specs=[VM, VM, VM], out_shape=[tab_shape, head_wire, tail_wire], scratch_shapes=[hold],
            compiler_params=params(GRANT), name="load")(small[0][0], small[0][1], small[0][2], ent_cols, ada_row, rel_tab)
        losses = []
        for step in range(rounds):
            to_owner, to_asker = ring(step)
            _, _, _, serve_rel, own_rel, key, rel_key, weight = small[step]
            far_tails = lax.ppermute(tails, 'ent', to_asker)
            far_heads = lax.ppermute(heads, 'ent', to_owner)
            tab, (give, loss) = call(
                head_kernel, "head_role", tab, [own_rel, rel_key, own_weight, heads, far_tails], [SM, SM, VM, VM, VM],
                [half_wire, shape(1)], [VM, SM], work, step_no=step)
            losses.append(loss)
            got = lax.ppermute(give, 'ent', away(1))
            tab, _ = call(
                tail_kernel, "tail_role", tab, [serve_rel, weight, far_heads, tails], [SM, VM, VM, VM],
                [], [], work + [pltpu.VMEM((edges, 512), F32)])
            tab, (own, *parts) = call(split_kernel, "rel_split", tab, [got], [VM], [part_wire] * 4, [VM] * 4)
            parts = [lax.ppermute(x, 'ent', away(2 * hop + 2)) for hop, x in enumerate(parts)]
            if step + 1 < rounds:
                nxt = small[step + 1]
                tab, (heads, tails) = call(
                    update_kernel, "update", tab, [key, nxt[0], nxt[1], nxt[2]], [SM] * 4, [head_wire, tail_wire], [VM, VM], [hold, hold])
            else:
                tab, _ = call(last_kernel, "last_update", tab, [key], [SM], [], [], [hold, hold])
            tab, (total,) = call(sum_kernel, "rel_sum", tab, [own, *parts], [VM] * 4, [part_wire], [VM])
            totals = [lax.ppermute(total, 'ent', away(2 * hop + 2)) for hop in range(3)]
            tab, (half,) = call(join_kernel, "rel_join", tab, [total, *totals], [VM] * 4, [half_wire], [VM])
            far_half = lax.ppermute(half, 'ent', away(1))
            tab, _ = call(rel_kernel, "rel_update", tab, [half, far_half], [VM] * 2, [], [])

        ent_out, ada_out, rel_tab = pl.pallas_call(
            functools.partial(store_kernel, areas=areas), grid=(part_rows // cols,), in_specs=[VM],
            out_specs=[pl.BlockSpec((DIM, cols), lambda i: (0, i)), pl.BlockSpec((1, cols), lambda i: (0, i)), ANY],
            out_shape=[shape(DIM, part_rows), shape(1, part_rows), shape(rel_rows, 4, LANES)], compiler_params=params(GRANT), name="store")(tab)
        ent_out, ada_out, rel_tab, losses = lax.optimization_barrier((ent_out, ada_out, rel_tab, losses))
        loss_out = jnp.concatenate(losses) / edges
        return ent_out.T, ada_out.reshape(part_rows), join_rows(rel_tab, rel_count), loss_out[None, :]

    return jax.shard_map(per_device, mesh=mesh, in_specs=(row_spec, state_spec, rel_spec, edge_spec, edge_spec, edge_spec, edge_spec, edge_spec), out_specs=(row_spec, state_spec, rel_spec, row_spec), check_vma=False)
```

```python
import functools

import jax
import jax.numpy as jnp
from jax import lax
from jax.experimental import pallas as pl
from jax.experimental.pallas import tpu as pltpu
from jax.sharding import PartitionSpec as P


LEARN_RATE = 0.25
ADA_EPS = 1e-10

DIM = 400
HALF = 200
ACC_LANE = 16
LANES = 128
MIB = 1 << 20
GRANT = 7

VM = pl.BlockSpec(memory_space=pltpu.VMEM)
SM = pl.BlockSpec(memory_space=pltpu.SMEM)
HBM = pl.BlockSpec(memory_space=pltpu.HBM)
F32 = jnp.float32
BF16 = jnp.bfloat16


def params(mib):
    return pltpu.CompilerParams(vmem_limit_bytes=mib * MIB)


def lane_ids(shape):
    return lax.broadcasted_iota(jnp.int32, shape, 1)


def swap_two(x):
    return pltpu.roll(x, 64, 1)


def swap_three(x):
    return jnp.where(lane_ids(x.shape) < 8, pltpu.roll(x, 120, 1), pltpu.roll(x, 8, 1))


def times(a, b):
    out = [a[0] * b[0] - a[1] * b[1], a[0] * b[1] + a[1] * b[0]]
    for x, y, swap, edge in ((a[2], b[2], swap_two, 64), (a[3], b[3], swap_three, 8)):
        xs, ys = swap(x), swap(y)
        out.append(jnp.where(lane_ids(x.shape) < edge, x * y - xs * ys, xs * y + x * ys))
    return out


def times_conj(a, b):
    out = [a[0] * b[0] + a[1] * b[1], a[1] * b[0] - a[0] * b[1]]
    for x, y, swap, edge in ((a[2], b[2], swap_two, 64), (a[3], b[3], swap_three, 8)):
        xs, ys = swap(x), swap(y)
        out.append(jnp.where(lane_ids(x.shape) < edge, x * y + xs * ys, x * ys - xs * y))
    return out


def keep_data(x):
    return jnp.where(lane_ids(x.shape) < ACC_LANE, x, 0.0)


def flat(ref):
    return ref.reshape(ref.shape[0] * 4, LANES)


def plane(ref2, start, rows, part):
    return ref2[pl.ds(start * 4 + part, rows, stride=4), :]


def put_plane(ref2, start, rows, part, x):
    ref2[pl.ds(start * 4 + part, rows, stride=4), :] = x


def copy_rows(idx_ref, count, src, dst, offset):
    def body(i, carry):
        dst[offset + i] = src[idx_ref[i]]
        return carry
    lax.fori_loop(0, count, body, 0, unroll=16)


def pack_rows(dst, src2, rows, first, groups, packed):
    step = rows // 8
    for g in range(groups):
        at, to = g * step, (first + g) * step
        for part in range(3):
            dst[part * rows + to:part * rows + to + step, :] = plane(src2, at, step, part).astype(dst.dtype)
        last = keep_data(plane(src2, at, step, 3))
        if first + g:
            last = pltpu.roll(last, 16 * (first + g), 1)
        packed = last if packed is None else packed + last
    if first + groups == 8:
        dst[3 * rows:3 * rows + step, :] = packed.astype(dst.dtype)
    return packed


def unpack_part(src, rows, g, step):
    planes = [src[part * rows + g * step:part * rows + (g + 1) * step, :].astype(F32) for part in range(3)]
    last = src[3 * rows:3 * rows + step, :].astype(F32)
    if g:
        last = pltpu.roll(last, LANES - 16 * g, 1)
    planes.append(keep_data(last))
    return planes


def row_parts(ent_ref, state, cols):
    return [
        ent_ref[0:128, :],
        ent_ref[HALF:HALF + 128, :],
        jnp.concatenate([ent_ref[128:192, :], ent_ref[HALF + 128:HALF + 192, :]], axis=0),
        jnp.concatenate([ent_ref[192:200, :], ent_ref[HALF + 192:HALF + 200, :], state, jnp.zeros((104, cols), F32)], axis=0),
    ]


def put_columns(ent_ref, x, part):
    if part < 2:
        ent_ref[part * HALF:part * HALF + 128, :] = x
    elif part == 2:
        ent_ref[128:192, :] = x[0:64]
        ent_ref[HALF + 128:HALF + 192, :] = x[64:128]
    else:
        ent_ref[192:200, :] = x[0:8]
        ent_ref[HALF + 192:HALF + 200, :] = x[8:16]


def load_kernel(ent_hbm, tab_ref, hold_ref, sems):
    cols = hold_ref.shape[2]
    blocks = ent_hbm.shape[1] // cols
    tab2 = flat(tab_ref)

    def fetch(b, slot):
        return pltpu.make_async_copy(ent_hbm.at[:, pl.ds(pl.multiple_of(b * cols, cols), cols)], hold_ref.at[slot], sems.at[slot])

    fetch(0, 0).start()

    def body(b, carry):
        slot = lax.rem(b, 2)
        fetch(b, slot).wait()

        @pl.when(b + 1 < blocks)
        def _():
            fetch(b + 1, 1 - slot).start()

        parts = row_parts(hold_ref.at[slot], jnp.zeros((8, cols), F32), cols)
        for part in range(4):
            tab2[pl.ds(b * (cols * 4) + part, cols, stride=4), :] = parts[part].T
        return carry

    lax.fori_loop(0, blocks, body, 0)


def load_rel_kernel(rel_ref, ada_ref, tab_ref, *, areas):
    tab2 = flat(tab_ref)
    block = 512

    def body(b, carry):
        state = jnp.broadcast_to(ada_ref[:, pl.ds(pl.multiple_of(b * block, block), block)], (LANES, block)).T
        at = pl.ds(b * (block * 4) + 3, block, stride=4)
        tab2[at, :] = jnp.where(lane_ids(state.shape) == ACC_LANE, state, tab2[at, :])
        return carry

    lax.fori_loop(0, ada_ref.shape[1] // block, body, 0)
    base, rows = areas['rel']
    count = rel_ref.shape[1]
    parts = row_parts(rel_ref, jnp.zeros((8, count), F32), count)
    for part in range(4):
        tab2[pl.ds(4 * base + part, count, stride=4), :] = parts[part].T
    tab_ref[base + count:base + rows] = jnp.zeros((rows - count, 4, LANES), F32)


def store_kernel(tab_ref, ent_ref, ada_ref):
    cols = ent_ref.shape[1]
    tab2 = flat(tab_ref)
    start = pl.program_id(0) * (cols * 4)
    for part in range(4):
        x = tab2[pl.ds(start + part, cols, stride=4), :].T
        put_columns(ent_ref, x, part)
        if part == 3:
            ada_ref[...] = x[ACC_LANE:ACC_LANE + 1]


def store_rel_kernel(tab_ref, rel_ref, *, areas):
    tab2 = flat(tab_ref)
    count = rel_ref.shape[1]
    for part in range(4):
        put_columns(rel_ref, tab2[pl.ds(4 * areas['rel'][0] + part, count, stride=4), :].T, part)


def gather_rows(head_ref, tail_ref, neg_ref, tab_ref, hold_ref, head_out, tail_out):
    edges = head_ref.shape[0]
    hold2 = flat(hold_ref)
    copy_rows(tail_ref, edges, tab_ref, hold_ref, 0)
    packed = pack_rows(tail_out, hold2, 2 * edges, 0, 4, None)
    copy_rows(neg_ref, edges, tab_ref, hold_ref, 0)
    pack_rows(tail_out, hold2, 2 * edges, 4, 4, packed)
    copy_rows(head_ref, edges, tab_ref, hold_ref, 0)
    pack_rows(head_out, hold2, edges, 0, 8, None)


def adagrad(grad, row):
    total = grad[0] * grad[0] + grad[1] * grad[1] + grad[2] * grad[2] + grad[3] * grad[3]
    mean = jnp.sum(total, axis=1, keepdims=True) * (1.0 / DIM)
    lane = lane_ids(row[3].shape)
    state = jnp.sum(jnp.where(lane == ACC_LANE, row[3], 0.0), axis=1, keepdims=True) + mean
    rate = LEARN_RATE / jnp.sqrt(state + ADA_EPS)
    new = [row[part] - grad[part] * rate for part in range(4)]
    new[3] = jnp.where(lane == ACC_LANE, state, new[3])
    return new


def apply_rows(key_ref, grad_ref, tab_ref, sum_ref, row_ref):
    size = sum_ref.shape[0]
    sum2, row2 = flat(sum_ref), flat(row_ref)
    block = 128

    def chunk(c, carry):
        base = c * size

        def collect(e, carry):
            prev, acc, old = carry
            key = key_ref[base + e]
            row = key >> 12
            same = row == prev
            g = grad_ref[key & 4095]
            acc = jnp.where(same, acc + g, g)
            old = jnp.where(same, old, tab_ref[row])
            sum_ref[e] = acc
            row_ref[e] = old
            return row, acc, old

        carry = lax.fori_loop(0, size, collect, carry, unroll=16)

        def update(b, carry):
            at = b * (block * 4)
            grad = [sum2[pl.ds(at + part, block, stride=4), :] for part in range(4)]
            row = [row2[pl.ds(at + part, block, stride=4), :] for part in range(4)]
            new = adagrad(grad, row)
            for part in range(4):
                row2[pl.ds(at + part, block, stride=4), :] = new[part]
            return carry

        lax.fori_loop(0, size // block, update, 0)

        def write(e, carry):
            tab_ref[key_ref[base + e] >> 12] = row_ref[e]
            return carry

        lax.fori_loop(0, size, write, 0, unroll=16)
        return carry

    zero = jnp.zeros((4, LANES), F32)
    lax.fori_loop(0, key_ref.shape[0] // size, chunk, (jnp.int32(-1), zero, zero))


def gather_kernel(head_ref, tail_ref, neg_ref, head_out, tail_out, tab_ref, hold_ref, *, areas):
    gather_rows(head_ref, tail_ref, neg_ref, tab_ref, hold_ref, head_out, tail_out)


def update_kernel(key_ref, tab_ref, sum_ref, row_ref, *, areas):
    apply_rows(key_ref, tab_ref.at[pl.ds(*areas['grad'])], tab_ref, sum_ref, row_ref)


def put_wide(ref, start, rows, planes):
    for part in range(4):
        ref[start:start + rows, part * LANES:(part + 1) * LANES] = planes[part].astype(ref.dtype)


def make_query(rel_ref, rel_tab, head_ref, tail_ref, hold_ref, query_ref, neg_ref):
    edges = rel_ref.shape[0]
    copy_rows(rel_ref, edges, rel_tab, hold_ref, 0)
    hold2 = flat(hold_ref)
    step = edges // 8
    wide = 2 * step
    for g in range(4):
        put_wide(neg_ref, g * wide, wide, unpack_part(tail_ref, 2 * edges, g + 4, wide))
    for g in range(8):
        heads = unpack_part(head_ref, edges, g, step)
        rels = [plane(hold2, g * step, step, part) for part in range(4)]
        rels[3] = keep_data(rels[3])
        put_wide(query_ref, g * step, step, times(heads, rels))
    return DIM ** -0.5


def tail_block(tail_ref, b, block):
    rows = 8 * block
    planes = [tail_ref[pl.ds(pl.multiple_of(part * rows + b * block, block), block), :].astype(F32) for part in range(3)]
    last = tail_ref[3 * rows:3 * rows + block, :].astype(F32)
    planes.append(keep_data(pltpu.roll(last, LANES - 16 * b, 1)))
    return planes


def head_kernel(rel_ref, key_ref, weight_ref, head_ref, tail_ref, give_out, loss_out, tab_ref, query_ref, neg_ref, *, areas, step_no):
    rel_tab, grad_out = tab_ref.at[pl.ds(*areas['rel'])], tab_ref.at[pl.ds(*areas['grad'])]
    edges = rel_ref.shape[0]
    hold_ref = grad_out.at[pl.ds(edges, edges)]
    scale = make_query(rel_ref, rel_tab, head_ref, tail_ref, hold_ref, query_ref, neg_ref)
    block = edges // 4

    def body(b, loss):
        at = pl.ds(pl.multiple_of(b * block, block), block)
        query = query_ref[at, :]
        tails = jnp.concatenate(tail_block(tail_ref, b, block), axis=1)
        pos = scale * jnp.sum(query * tails, axis=1, keepdims=True)
        neg = scale * lax.dot_general(query.astype(BF16), neg_ref[...], (((1,), (1,)), ((), ())), preferred_element_type=F32)
        top = jnp.maximum(pos, jnp.max(neg, axis=1, keepdims=True))
        pos_exp = jnp.exp(pos - top)
        neg_exp = jnp.exp(neg - top)
        denom = pos_exp + jnp.sum(neg_exp, axis=1, keepdims=True)
        weight = weight_ref[at, step_no:step_no + 1]
        loss = loss + weight * (top + jnp.log(denom) - pos)
        d_pos = weight * (pos_exp / denom - 1.0)
        d_neg = ((weight / denom) * neg_exp).astype(BF16)
        query_ref[at, :] = scale * (d_pos * tails + jnp.dot(d_neg, neg_ref[...], preferred_element_type=F32))
        return loss

    loss = lax.fori_loop(0, edges // block, body, jnp.zeros((block, 1), F32))
    loss_out[0] = jnp.sum(loss)
    hold2, grad2 = flat(hold_ref), flat(grad_out)
    step = edges // 8
    for g in range(8):
        at = g * step
        heads = unpack_part(head_ref, edges, g, step)
        rels = [plane(hold2, at, step, part) for part in range(4)]
        rels[3] = keep_data(rels[3])
        d_query = [query_ref[at:at + step, part * LANES:(part + 1) * LANES] for part in range(4)]
        d_head = times_conj(d_query, rels)
        d_rel = times_conj(d_query, heads)
        for part in range(4):
            put_plane(grad2, at, step, part, d_head[part])
            put_plane(hold2, at, step, part, d_rel[part])

    rel_rows = rel_tab.shape[0]
    sum_ref = grad_out.at[pl.ds(2 * edges, rel_rows)]
    sum_ref[...] = jnp.zeros(sum_ref.shape, F32)

    def scatter(e, carry):
        prev, acc = carry
        key = key_ref[e]
        row = key >> 10
        g = hold_ref[key & 1023]
        acc = jnp.where(row == prev, acc + g, g)
        sum_ref[row] = acc
        return row, acc

    lax.fori_loop(0, edges, scatter, (jnp.int32(-1), jnp.zeros((4, LANES), F32)), unroll=16)
    drel_out = flat(tab_ref.at[pl.ds(*areas['drel'])])
    pack_rows(drel_out, flat(sum_ref), rel_rows, 0, 8, None)
    used, half = rel_rows * 25 // 8, give_out.shape[0]
    drel_out[used:, :] = jnp.zeros((2 * half - used, LANES), F32)
    core = lax.rem(lax.axis_index('ent'), 2)
    give_out[...] = drel_out[pl.ds(pl.multiple_of((1 - core) * half, 8), half), :]


def tail_kernel(rel_ref, weight_ref, head_ref, tail_ref, tab_ref, query_ref, neg_ref, sum_ref, *, areas):
    rel_tab, grad_out = tab_ref.at[pl.ds(*areas['rel'])], tab_ref.at[pl.ds(*areas['grad'])]
    edges = rel_ref.shape[0]
    hold_ref = grad_out.at[pl.ds(edges, edges)]
    scale = make_query(rel_ref, rel_tab, head_ref, tail_ref, hold_ref, query_ref, neg_ref)
    block = edges // 4
    grad2 = flat(grad_out)
    sum_ref[...] = jnp.zeros(sum_ref.shape, F32)

    def body(b, carry):
        at = pl.ds(pl.multiple_of(b * block, block), block)
        query = query_ref[at, :]
        query_bf = query.astype(BF16)
        tails = tail_block(tail_ref, b, block)
        prod = [query[:, part * LANES:(part + 1) * LANES] * tails[part] for part in range(4)]
        prod = (prod[0] + prod[1]) + (prod[2] + prod[3])
        pos = scale * jnp.sum(prod.T, axis=0, keepdims=True)
        neg = scale * lax.dot_general(neg_ref[...], query_bf, (((1,), (1,)), ((), ())), preferred_element_type=F32)
        top = jnp.maximum(pos, jnp.max(neg, axis=0, keepdims=True))
        pos_exp = jnp.exp(pos - top)
        neg_exp = jnp.exp(neg - top)
        denom = pos_exp + jnp.sum(neg_exp, axis=0, keepdims=True)
        weight = weight_ref[pl.ds(b, 1), :]
        d_pos = weight * (pos_exp / denom - 1.0)
        d_neg = ((weight / denom) * neg_exp).astype(BF16)
        sum_ref[...] += jnp.dot(d_neg, query_bf, preferred_element_type=F32)
        d_pos_col = jnp.broadcast_to(d_pos, (LANES, block)).T
        for part in range(4):
            grad2[pl.ds((edges + b * block) * 4 + part, block, stride=4), :] = scale * d_pos_col * query[:, part * LANES:(part + 1) * LANES]
        return carry

    lax.fori_loop(0, edges // block, body, 0)
    for part in range(4):
        put_plane(grad2, 2 * edges, edges, part, scale * sum_ref[:, part * LANES:(part + 1) * LANES])


def split_kernel(got_ref, own_out, one_out, two_out, three_out, tab_ref, *, areas):
    drel_ref = flat(tab_ref.at[pl.ds(*areas['drel'])])
    half, piece = got_ref.shape[0], own_out.shape[0]
    me = lax.axis_index('ent')
    core, chip = lax.rem(me, 2), lax.div(me, 2)
    for away, out in enumerate((own_out, one_out, two_out, three_out)):
        at = pl.multiple_of((chip ^ away) * piece, 8)
        out[...] = drel_ref[pl.ds(pl.multiple_of(core * half + at, 8), piece), :] + got_ref[pl.ds(at, piece), :]


def sum_kernel(own_ref, one_ref, two_ref, three_ref, out, tab_ref, *, areas):
    out[...] = (own_ref[...] + one_ref[...]) + (two_ref[...] + three_ref[...])


def join_kernel(own_ref, one_ref, two_ref, three_ref, out, tab_ref, *, areas):
    piece = own_ref.shape[0]
    chip = lax.div(lax.axis_index('ent'), 2)
    for away, ref in enumerate((own_ref, one_ref, two_ref, three_ref)):
        out[pl.ds(pl.multiple_of((chip ^ away) * piece, 8), piece), :] = ref[...]


def rel_kernel(half_ref, far_ref, tab_ref, *, areas):
    drel_ref = flat(tab_ref.at[pl.ds(*areas['drel'])])
    rel_tab = tab_ref.at[pl.ds(*areas['rel'])]
    rows = rel_tab.shape[0]
    half = half_ref.shape[0]
    core = lax.rem(lax.axis_index('ent'), 2)
    drel_ref[pl.ds(pl.multiple_of(core * half, 8), half), :] = half_ref[...]
    drel_ref[pl.ds(pl.multiple_of((1 - core) * half, 8), half), :] = far_ref[...]
    step = rows // 8
    rel2 = flat(rel_tab)
    for g in range(8):
        grad = unpack_part(drel_ref, rows, g, step)
        row = [plane(rel2, g * step, step, part) for part in range(4)]
        new = adagrad(grad, row)
        for part in range(4):
            put_plane(rel2, g * step, step, part, new[part])


def shape(*dims, dtype=F32):
    return jax.ShapeDtypeStruct(dims, dtype)


def solution(mesh):
    ent_devs = mesh.shape['ent']
    row_spec = P(('sweep', 'ent'), None)
    state_spec = P(('sweep', 'ent'))
    rel_spec = P('sweep', None)
    edge_spec = P(('sweep', 'ent'), None, None)

    def per_device(ent_part, ada_part, rel_table, head_idx, tail_idx, rel_idx, neg_idx, edge_mask):
        part_rows = ent_part.shape[0]
        rel_count = rel_table.shape[0]
        rounds = head_idx.shape[1]
        edges = head_idx.shape[2]
        rel_rows = -(-rel_count // 128) * 128
        head_idx, tail_idx, rel_idx, neg_idx, edge_mask = (x[0] for x in (head_idx, tail_idx, rel_idx, neg_idx, edge_mask))

        piece = -(-(rel_rows * 25 // 8) // 64) * 8

        def away(bits):
            return [(sender, sender ^ bits) for sender in range(ent_devs)]

        def ring(step):
            shift = step + 1
            to_owner = [(sender, (sender + shift) % ent_devs) for sender in range(ent_devs)]
            return to_owner, [(target, sender) for sender, target in to_owner]

        asked = jnp.stack([tail_idx, neg_idx, rel_idx, edge_mask], axis=1)
        served = jnp.stack([lax.ppermute(asked[step], 'ent', ring(step)[0]) for step in range(rounds)])
        rows_all = jnp.concatenate([head_idx, served[:, 0], served[:, 1]], axis=1)
        keys = lax.sort(rows_all * 4096 + jnp.arange(3 * edges, dtype=jnp.int32)[None, :], dimension=1, is_stable=False)
        rel_keys = lax.sort(rel_idx * 1024 + jnp.arange(edges, dtype=jnp.int32)[None, :], dimension=1, is_stable=False)
        own_weight = jnp.pad(edge_mask.astype(F32), ((0, 8 - rounds), (0, 0))).T
        serve_weight = served[:, 3].astype(F32).reshape(rounds, edges // 256, 256)
        small = []
        for step in range(rounds):
            small.append((head_idx[step], served[step, 0], served[step, 1], served[step, 2], rel_idx[step], keys[step], rel_keys[step], serve_weight[step]))
        small, own_weight, rel_cols, ent_cols, ada_row = lax.optimization_barrier((small, own_weight, rel_table.T, ent_part.T, ada_part.reshape(1, part_rows)))

        cols = 512
        grad_rows = 2 * edges + max(edges, rel_rows)
        areas = {'grad': (part_rows, grad_rows), 'rel': (part_rows + grad_rows, rel_rows), 'drel': (part_rows + grad_rows + rel_rows, 2 * piece)}
        tab_shape = pltpu.VMEM((sum(areas['drel']), 4, LANES), F32)
        head_wire, tail_wire = shape(edges * 25 // 8, LANES), shape(2 * edges * 25 // 8, LANES, dtype=BF16)
        part_wire, half_wire = shape(piece, LANES), shape(4 * piece, LANES)
        hold = pltpu.VMEM((edges, 4, LANES), F32)
        work = [pltpu.VMEM((edges, 512), F32), pltpu.VMEM((edges, 512), BF16)]

        def call(kernel, name, tab, inputs, in_specs, out_shape, out_specs, scratch=(), **more):
            ins, outs = len(inputs), len(out_shape)

            def body(*refs):
                kernel(*refs[:ins], *refs[ins + 2:ins + 2 + outs], refs[ins + 1], *refs[ins + 2 + outs:], areas=areas, **more)

            got = pl.pallas_call(
                body, in_specs=in_specs + [VM], out_specs=[VM] + out_specs, out_shape=[tab_shape] + out_shape,
                input_output_aliases={ins: 0}, scratch_shapes=list(scratch), compiler_params=params(GRANT), name=name)(*inputs, tab)
            return got[0], got[1:]

        tab = pl.pallas_call(
            load_kernel, in_specs=[HBM], out_specs=VM, out_shape=tab_shape,
            scratch_shapes=[pltpu.VMEM((2, DIM, cols), F32), pltpu.SemaphoreType.DMA((2,))],
            compiler_params=params(GRANT), name="load")(ent_cols)
        tab, _ = call(load_rel_kernel, "load_rel", tab, [rel_cols, ada_row], [VM, VM], [], [])
        losses = []
        half = None
        for step in range(rounds):
            to_owner, to_asker = ring(step)
            head_ids, serve_tails, serve_negs, serve_rel, own_rel, key, rel_key, weight = small[step]
            tab, (heads, tails) = call(
                gather_kernel, "gather", tab, [head_ids, serve_tails, serve_negs], [SM] * 3, [head_wire, tail_wire], [VM, VM], [hold])
            far_tails = lax.ppermute(tails, 'ent', to_asker)
            far_heads = lax.ppermute(heads, 'ent', to_owner)
            if step:
                tab, _ = call(rel_kernel, "rel_update", tab, [half, far_half], [VM] * 2, [], [])
            tab, (give, loss) = call(
                head_kernel, "head_role", tab, [own_rel, rel_key, own_weight, heads, far_tails], [SM, SM, VM, VM, VM],
                [half_wire, shape(1)], [VM, SM], work, step_no=step)
            losses.append(loss)
            got = lax.ppermute(give, 'ent', away(1))
            tab, (own, *parts) = call(split_kernel, "rel_split", tab, [got], [VM], [part_wire] * 4, [VM] * 4)
            parts = [lax.ppermute(x, 'ent', away(2 * hop + 2)) for hop, x in enumerate(parts)]
            tab, _ = call(
                tail_kernel, "tail_role", tab, [serve_rel, weight, far_heads, tails], [SM, VM, VM, VM],
                [], [], work + [pltpu.VMEM((edges, 512), F32)])
            tab, (total,) = call(sum_kernel, "rel_sum", tab, [own, *parts], [VM] * 4, [part_wire], [VM])
            totals = [lax.ppermute(total, 'ent', away(2 * hop + 2)) for hop in range(3)]
            tab, _ = call(update_kernel, "update", tab, [key], [SM], [], [], [hold, hold])
            tab, (half,) = call(join_kernel, "rel_join", tab, [total, *totals], [VM] * 4, [half_wire], [VM])
            far_half = lax.ppermute(half, 'ent', away(1))
        tab, _ = call(rel_kernel, "rel_update", tab, [half, far_half], [VM] * 2, [], [])

        ent_out, ada_out = pl.pallas_call(
            store_kernel, grid=(part_rows // cols,), in_specs=[VM],
            out_specs=[pl.BlockSpec((DIM, cols), lambda i: (0, i)), pl.BlockSpec((1, cols), lambda i: (0, i))],
            out_shape=[shape(DIM, part_rows), shape(1, part_rows)], compiler_params=params(GRANT), name="store")(tab)
        rel_out = pl.pallas_call(
            functools.partial(store_rel_kernel, areas=areas), in_specs=[VM], out_specs=VM,
            out_shape=shape(DIM, rel_count), compiler_params=params(GRANT), name="store_rel")(tab)
        ent_out, ada_out, rel_out, losses = lax.optimization_barrier((ent_out, ada_out, rel_out, losses))
        loss_out = jnp.concatenate(losses) / edges
        return ent_out.T, ada_out.reshape(part_rows), rel_out.T, loss_out[None, :]

    return jax.shard_map(per_device, mesh=mesh, in_specs=(row_spec, state_spec, rel_spec, edge_spec, edge_spec, edge_spec, edge_spec, edge_spec), out_specs=(row_spec, state_spec, rel_spec, row_spec), check_vma=False)
```

```python
import functools

import jax
import jax.numpy as jnp
from jax import lax
from jax.experimental import pallas as pl
from jax.experimental.pallas import tpu as pltpu
from jax.sharding import PartitionSpec as P


LEARN_RATE = 0.25
ADA_EPS = 1e-10

DIM = 400
HALF = 200
ACC_LANE = 16
LANES = 128
MIB = 1 << 20
GRANT = 7
TAILS_FIRST = (True, False)

VM = pl.BlockSpec(memory_space=pltpu.VMEM)
SM = pl.BlockSpec(memory_space=pltpu.SMEM)
HBM = pl.BlockSpec(memory_space=pltpu.HBM)
F32 = jnp.float32
BF16 = jnp.bfloat16


def params(mib):
    return pltpu.CompilerParams(vmem_limit_bytes=mib * MIB)


def lane_ids(shape):
    return lax.broadcasted_iota(jnp.int32, shape, 1)


def swap_two(x):
    return pltpu.roll(x, 64, 1)


def swap_three(x):
    return jnp.where(lane_ids(x.shape) < 8, pltpu.roll(x, 120, 1), pltpu.roll(x, 8, 1))


def times(a, b):
    out = [a[0] * b[0] - a[1] * b[1], a[0] * b[1] + a[1] * b[0]]
    for x, y, swap, edge in ((a[2], b[2], swap_two, 64), (a[3], b[3], swap_three, 8)):
        xs, ys = swap(x), swap(y)
        out.append(jnp.where(lane_ids(x.shape) < edge, x * y - xs * ys, xs * y + x * ys))
    return out


def times_conj(a, b):
    out = [a[0] * b[0] + a[1] * b[1], a[1] * b[0] - a[0] * b[1]]
    for x, y, swap, edge in ((a[2], b[2], swap_two, 64), (a[3], b[3], swap_three, 8)):
        xs, ys = swap(x), swap(y)
        out.append(jnp.where(lane_ids(x.shape) < edge, x * y + xs * ys, x * ys - xs * y))
    return out


def keep_data(x):
    return jnp.where(lane_ids(x.shape) < ACC_LANE, x, 0.0)


def flat(ref):
    return ref.reshape(ref.shape[0] * 4, LANES)


def plane(ref2, start, rows, part):
    return ref2[pl.ds(start * 4 + part, rows, stride=4), :]


def put_plane(ref2, start, rows, part, x):
    ref2[pl.ds(start * 4 + part, rows, stride=4), :] = x


def copy_rows(idx_ref, count, src, dst, offset):
    def body(i, carry):
        dst[offset + i] = src[idx_ref[i]]
        return carry

    lax.fori_loop(0, count, body, 0, unroll=16)


def pack_rows(dst, src2, rows, first, groups, packed):
    step = rows // 8
    for g in range(groups):
        at, to = g * step, (first + g) * step
        for part in range(3):
            dst[part * rows + to:part * rows + to + step, :] = plane(src2, at, step, part).astype(dst.dtype)
        last = keep_data(plane(src2, at, step, 3))
        if first + g:
            last = pltpu.roll(last, 16 * (first + g), 1)
        packed = last if packed is None else packed + last
    if first + groups == 8:
        dst[3 * rows:3 * rows + step, :] = packed.astype(dst.dtype)
    return packed


def unpack_part(src, rows, g, step):
    planes = [src[part * rows + g * step:part * rows + (g + 1) * step, :].astype(F32) for part in range(3)]
    last = src[3 * rows:3 * rows + step, :].astype(F32)
    if g:
        last = pltpu.roll(last, LANES - 16 * g, 1)
    planes.append(keep_data(last))
    return planes


def row_parts(ent_ref, state, cols):
    return [
        ent_ref[0:128, :],
        ent_ref[HALF:HALF + 128, :],
        jnp.concatenate([ent_ref[128:192, :], ent_ref[HALF + 128:HALF + 192, :]], axis=0),
        jnp.concatenate([ent_ref[192:200, :], ent_ref[HALF + 192:HALF + 200, :], state, jnp.zeros((104, cols), F32)], axis=0),
    ]


def put_columns(ent_ref, x, part):
    if part < 2:
        ent_ref[part * HALF:part * HALF + 128, :] = x
    elif part == 2:
        ent_ref[128:192, :] = x[0:64]
        ent_ref[HALF + 128:HALF + 192, :] = x[64:128]
    else:
        ent_ref[192:200, :] = x[0:8]
        ent_ref[HALF + 192:HALF + 200, :] = x[8:16]


def load_kernel(ent_hbm, tab_ref, hold_ref, sems):
    cols = hold_ref.shape[2]
    blocks = ent_hbm.shape[1] // cols
    tab2 = flat(tab_ref)

    def fetch(b, slot):
        return pltpu.make_async_copy(ent_hbm.at[:, pl.ds(pl.multiple_of(b * cols, cols), cols)], hold_ref.at[slot], sems.at[slot])

    slots = hold_ref.shape[0]
    for b in range(slots - 1):
        fetch(b, b).start()

    def body(b, carry):
        slot = lax.rem(b, slots)
        fetch(b, slot).wait()
        ahead = b + slots - 1

        @pl.when(ahead < blocks)
        def _():
            fetch(ahead, lax.rem(ahead, slots)).start()

        parts = row_parts(hold_ref.at[slot], jnp.zeros((8, cols), F32), cols)
        for part in range(4):
            tab2[pl.ds(b * (cols * 4) + part, cols, stride=4), :] = parts[part].T
        return carry

    lax.fori_loop(0, blocks, body, 0)


def load_rel_kernel(rel_ref, ada_ref, tab_ref, *, areas):
    tab2 = flat(tab_ref)
    block = 512

    def body(b, carry):
        state = jnp.broadcast_to(ada_ref[:, pl.ds(pl.multiple_of(b * block, block), block)], (LANES, block)).T
        at = pl.ds(b * (block * 4) + 3, block, stride=4)
        tab2[at, :] = jnp.where(lane_ids(state.shape) == ACC_LANE, state, tab2[at, :])
        return carry

    lax.fori_loop(0, ada_ref.shape[1] // block, body, 0)
    base, rows = areas['rel']
    count = rel_ref.shape[1]
    parts = row_parts(rel_ref, jnp.zeros((8, count), F32), count)
    for part in range(4):
        tab2[pl.ds(4 * base + part, count, stride=4), :] = parts[part].T
    tab_ref[base + count:base + rows] = jnp.zeros((rows - count, 4, LANES), F32)


def store_kernel(tab_ref, ent_ref, ada_ref):
    cols = ent_ref.shape[1]
    tab2 = flat(tab_ref)
    start = pl.program_id(0) * (cols * 4)
    for part in range(4):
        x = tab2[pl.ds(start + part, cols, stride=4), :].T
        put_columns(ent_ref, x, part)
        if part == 3:
            ada_ref[...] = x[ACC_LANE:ACC_LANE + 1]


def store_rel_kernel(tab_ref, rel_ref, loss_ref, *, areas, edges):
    tab2 = flat(tab_ref)
    count = rel_ref.shape[1]
    for part in range(4):
        put_columns(rel_ref, tab2[pl.ds(4 * areas['rel'][0] + part, count, stride=4), :].T, part)
    base, rounds = areas['loss']
    lane = lane_ids((1, LANES))
    total = jnp.zeros((1, LANES), F32)
    for step in range(rounds):
        total = jnp.where(lane == step, tab2[4 * (base + step):4 * (base + step) + 1, :], total)
    loss_ref[...] = total * (1.0 / edges)


def gather_tails_kernel(tail_ref, neg_ref, tail_out, tab_ref, hold_ref, *, areas):
    edges = tail_ref.shape[0]
    hold2 = flat(hold_ref)
    copy_rows(tail_ref, edges, tab_ref, hold_ref, 0)
    packed = pack_rows(tail_out, hold2, 2 * edges, 0, 4, None)
    copy_rows(neg_ref, edges, tab_ref, hold_ref, 0)
    pack_rows(tail_out, hold2, 2 * edges, 4, 4, packed)


def gather_heads_kernel(head_ref, one_out, two_out, tab_ref, hold_ref, *, areas):
    edges = head_ref.shape[0]
    copy_rows(head_ref, edges, tab_ref, hold_ref, 0)
    for side, out in enumerate((one_out, two_out)):
        half = hold_ref.at[pl.ds(side * (edges // 2), edges // 2)]
        pack_rows(out, flat(half), edges // 2, 0, 8, None)


def adagrad(grad, row):
    total = grad[0] * grad[0] + grad[1] * grad[1] + grad[2] * grad[2] + grad[3] * grad[3]
    mean = jnp.sum(total, axis=1, keepdims=True) * (1.0 / DIM)
    lane = lane_ids(row[3].shape)
    state = jnp.sum(jnp.where(lane == ACC_LANE, row[3], 0.0), axis=1, keepdims=True) + mean
    rate = LEARN_RATE / jnp.sqrt(state + ADA_EPS)
    new = [row[part] - grad[part] * rate for part in range(4)]
    new[3] = jnp.where(lane == ACC_LANE, state, new[3])
    return new


def apply_rows(key_ref, grad_ref, tab_ref, sum_ref, row_ref):
    size = sum_ref.shape[0]
    sum2, row2 = flat(sum_ref), flat(row_ref)
    block = 128

    def chunk(c, carry):
        base = c * size

        def collect(e, carry):
            prev, acc, old = carry
            key = key_ref[base + e]
            row = key >> 12
            same = row == prev
            g = grad_ref[key & 4095]
            acc = jnp.where(same, acc + g, g)
            old = jnp.where(same, old, tab_ref[row])
            sum_ref[e] = acc
            row_ref[e] = old
            return row, acc, old

        carry = lax.fori_loop(0, size, collect, carry, unroll=16)

        def update(b, carry):
            at = b * (block * 4)
            grad = [sum2[pl.ds(at + part, block, stride=4), :] for part in range(4)]
            row = [row2[pl.ds(at + part, block, stride=4), :] for part in range(4)]
            new = adagrad(grad, row)
            for part in range(4):
                row2[pl.ds(at + part, block, stride=4), :] = new[part]
            return carry

        lax.fori_loop(0, size // block, update, 0)

        def write(e, carry):
            tab_ref[key_ref[base + e] >> 12] = row_ref[e]
            return carry

        lax.fori_loop(0, size, write, 0, unroll=16)
        return carry

    zero = jnp.zeros((4, LANES), F32)
    lax.fori_loop(0, key_ref.shape[0] // size, chunk, (jnp.int32(-1), zero, zero))


def update_kernel(key_ref, tab_ref, sum_ref, row_ref, *, areas):
    apply_rows(key_ref, tab_ref.at[pl.ds(*areas['grad'])], tab_ref, sum_ref, row_ref)


def put_wide(ref, start, rows, planes):
    for part in range(4):
        ref[start:start + rows, part * LANES:(part + 1) * LANES] = planes[part].astype(ref.dtype)


def unpack_negs(tail_ref, neg_ref):
    edges = neg_ref.shape[0]
    wide = edges // 4
    for g in range(4):
        put_wide(neg_ref, g * wide, wide, unpack_part(tail_ref, 2 * edges, g + 4, wide))


def put_queries(head_ref, hold2, query_ref, start):
    rows = head_ref.shape[0] * 8 // 25
    step = rows // 8
    for g in range(8):
        heads = unpack_part(head_ref, rows, g, step)
        rels = [plane(hold2, start + g * step, step, part) for part in range(4)]
        rels[3] = keep_data(rels[3])
        put_wide(query_ref, start + g * step, step, times(heads, rels))


def tail_block(tail_ref, b, block):
    rows = 8 * block
    planes = [tail_ref[pl.ds(pl.multiple_of(part * rows + b * block, block), block), :].astype(F32) for part in range(3)]
    last = tail_ref[3 * rows:3 * rows + block, :].astype(F32)
    planes.append(keep_data(pltpu.roll(last, LANES - 16 * b, 1)))
    return planes


def head_kernel(rel_ref, key_ref, weight_ref, one_ref, two_ref, tail_ref, give_out, tab_ref, query_ref, neg_ref, *, areas, step_no):
    rel_tab, grad_out = tab_ref.at[pl.ds(*areas['rel'])], tab_ref.at[pl.ds(*areas['grad'])]
    edges = rel_ref.shape[0]
    hold_ref = grad_out.at[pl.ds(edges, edges)]
    copy_rows(rel_ref, edges, rel_tab, hold_ref, 0)
    unpack_negs(tail_ref, neg_ref)
    scale = DIM ** -0.5
    for side, head_ref in enumerate((one_ref, two_ref)):
        put_queries(head_ref, flat(hold_ref), query_ref, side * (edges // 2))
    block = edges // 4

    def body(b, loss):
        at = pl.ds(pl.multiple_of(b * block, block), block)
        query = query_ref[at, :]
        tails = jnp.concatenate(tail_block(tail_ref, b, block), axis=1)
        pos = scale * jnp.sum(query * tails, axis=1, keepdims=True)
        neg = scale * lax.dot_general(query.astype(BF16), neg_ref[...], (((1,), (1,)), ((), ())), preferred_element_type=F32)
        top = jnp.maximum(pos, jnp.max(neg, axis=1, keepdims=True))
        pos_exp = jnp.exp(pos - top)
        neg_exp = jnp.exp(neg - top)
        denom = pos_exp + jnp.sum(neg_exp, axis=1, keepdims=True)
        weight = weight_ref[at, step_no:step_no + 1]
        loss = loss + weight * (top + jnp.log(denom) - pos)
        d_pos = weight * (pos_exp / denom - 1.0)
        d_neg = ((weight / denom) * neg_exp).astype(BF16)
        query_ref[at, :] = scale * (d_pos * tails + jnp.dot(d_neg, neg_ref[...], preferred_element_type=F32))
        return loss

    loss = lax.fori_loop(0, edges // block, body, jnp.zeros((block, 1), F32))
    tab_ref[areas['loss'][0] + step_no] = jnp.broadcast_to(jnp.sum(loss, axis=0, keepdims=True), (4, LANES))
    hold2, grad2 = flat(hold_ref), flat(grad_out)
    half = edges // 2
    step = half // 8
    for side, head_ref in enumerate((one_ref, two_ref)):
        for g in range(8):
            at = side * half + g * step
            heads = unpack_part(head_ref, half, g, step)
            rels = [plane(hold2, at, step, part) for part in range(4)]
            rels[3] = keep_data(rels[3])
            d_query = [query_ref[at:at + step, part * LANES:(part + 1) * LANES] for part in range(4)]
            d_head = times_conj(d_query, rels)
            d_rel = times_conj(d_query, heads)
            for part in range(4):
                put_plane(grad2, at, step, part, d_head[part])
                put_plane(hold2, at, step, part, d_rel[part])

    rel_rows = rel_tab.shape[0]
    sum_ref = grad_out.at[pl.ds(2 * edges, rel_rows)]
    sum_ref[...] = jnp.zeros(sum_ref.shape, F32)

    def scatter(e, carry):
        prev, acc = carry
        key = key_ref[e]
        row = key >> 10
        g = hold_ref[key & 1023]
        acc = jnp.where(row == prev, acc + g, g)
        sum_ref[row] = acc
        return row, acc

    lax.fori_loop(0, edges, scatter, (jnp.int32(-1), jnp.zeros((4, LANES), F32)), unroll=16)
    drel_out = flat(tab_ref.at[pl.ds(*areas['drel'])])
    pack_rows(drel_out, flat(sum_ref), rel_rows, 0, 8, None)
    used, half = rel_rows * 25 // 8, give_out.shape[0]
    drel_out[used:, :] = jnp.zeros((2 * half - used, LANES), F32)
    core = lax.rem(lax.axis_index('ent'), 2)
    give_out[...] = drel_out[pl.ds(pl.multiple_of((1 - core) * half, 8), half), :]


def tail_kernel(rel_ref, weight_ref, head_ref, tail_ref, tab_ref, query_ref, neg_ref, sum_ref, *, areas, side, last):
    rel_tab, grad_out = tab_ref.at[pl.ds(*areas['rel'])], tab_ref.at[pl.ds(*areas['grad'])]
    edges = neg_ref.shape[0]
    half = edges // 2
    hold_ref = grad_out.at[pl.ds(edges + side * half, half)]
    unpack_negs(tail_ref, neg_ref)

    def fetch(i, carry):
        hold_ref[i] = rel_tab[rel_ref[side * half + i]]
        return carry

    lax.fori_loop(0, half, fetch, 0, unroll=16)
    put_queries(head_ref, flat(hold_ref), query_ref, 0)
    scale = DIM ** -0.5
    block = edges // 4
    grad2 = flat(grad_out)
    sum_ref[...] = jnp.zeros(sum_ref.shape, F32)

    def body(b, carry):
        at = pl.ds(pl.multiple_of(b * block, block), block)
        query = query_ref[at, :]
        query_bf = query.astype(BF16)
        tails = tail_block(tail_ref, b + 2 * side, block)
        prod = [query[:, part * LANES:(part + 1) * LANES] * tails[part] for part in range(4)]
        prod = (prod[0] + prod[1]) + (prod[2] + prod[3])
        pos = scale * jnp.sum(prod.T, axis=0, keepdims=True)
        neg = scale * lax.dot_general(neg_ref[...], query_bf, (((1,), (1,)), ((), ())), preferred_element_type=F32)
        top = jnp.maximum(pos, jnp.max(neg, axis=0, keepdims=True))
        pos_exp = jnp.exp(pos - top)
        neg_exp = jnp.exp(neg - top)
        denom = pos_exp + jnp.sum(neg_exp, axis=0, keepdims=True)
        weight = weight_ref[pl.ds(b + 2 * side, 1), :]
        d_pos = weight * (pos_exp / denom - 1.0)
        d_neg = ((weight / denom) * neg_exp).astype(BF16)
        sum_ref[...] += jnp.dot(d_neg, query_bf, preferred_element_type=F32)
        d_pos_col = jnp.broadcast_to(d_pos, (LANES, block)).T
        for part in range(4):
            grad2[pl.ds((edges + side * half + b * block) * 4 + part, block, stride=4), :] = scale * d_pos_col * query[:, part * LANES:(part + 1) * LANES]
        return carry

    lax.fori_loop(0, half // block, body, 0)
    for part in range(4):
        total = scale * sum_ref[:, part * LANES:(part + 1) * LANES]
        if last:
            total = total + plane(grad2, 2 * edges, edges, part)
        put_plane(grad2, 2 * edges, edges, part, total)


def split_kernel(got_ref, own_out, one_out, two_out, three_out, tab_ref, *, areas):
    drel_ref = flat(tab_ref.at[pl.ds(*areas['drel'])])
    half, piece = got_ref.shape[0], own_out.shape[0]
    me = lax.axis_index('ent')
    core, chip = lax.rem(me, 2), lax.div(me, 2)
    for away, out in enumerate((own_out, one_out, two_out, three_out)):
        at = pl.multiple_of((chip ^ away) * piece, 8)
        out[...] = drel_ref[pl.ds(pl.multiple_of(core * half + at, 8), piece), :] + got_ref[pl.ds(at, piece), :]


def sum_kernel(own_ref, one_ref, two_ref, three_ref, out, tab_ref, *, areas):
    out[...] = (own_ref[...] + one_ref[...]) + (two_ref[...] + three_ref[...])


def join_kernel(own_ref, one_ref, two_ref, three_ref, out, tab_ref, *, areas):
    piece = own_ref.shape[0]
    chip = lax.div(lax.axis_index('ent'), 2)
    for away, ref in enumerate((own_ref, one_ref, two_ref, three_ref)):
        out[pl.ds(pl.multiple_of((chip ^ away) * piece, 8), piece), :] = ref[...]


def rel_kernel(half_ref, far_ref, tab_ref, *, areas):
    drel_ref = flat(tab_ref.at[pl.ds(*areas['drel'])])
    rel_tab = tab_ref.at[pl.ds(*areas['rel'])]
    rows = rel_tab.shape[0]
    half = half_ref.shape[0]
    core = lax.rem(lax.axis_index('ent'), 2)
    drel_ref[pl.ds(pl.multiple_of(core * half, 8), half), :] = half_ref[...]
    drel_ref[pl.ds(pl.multiple_of((1 - core) * half, 8), half), :] = far_ref[...]
    step = rows // 8
    rel2 = flat(rel_tab)
    for g in range(8):
        grad = unpack_part(drel_ref, rows, g, step)
        row = [plane(rel2, g * step, step, part) for part in range(4)]
        new = adagrad(grad, row)
        for part in range(4):
            put_plane(rel2, g * step, step, part, new[part])


def shape(*dims, dtype=F32):
    return jax.ShapeDtypeStruct(dims, dtype)


def solution(mesh):
    ent_devs = mesh.shape['ent']
    row_spec = P(('sweep', 'ent'), None)
    state_spec = P(('sweep', 'ent'))
    rel_spec = P('sweep', None)
    edge_spec = P(('sweep', 'ent'), None, None)

    def train(ent_part, ada_part, rel_table, head_idx, tail_idx, rel_idx, neg_idx, edge_mask):
        part_rows = ent_part.shape[0]
        rel_count = rel_table.shape[0]
        rounds = head_idx.shape[1]
        edges = head_idx.shape[2]
        rel_rows = -(-rel_count // 128) * 128
        head_idx, tail_idx, rel_idx, neg_idx, edge_mask = (x[0] for x in (head_idx, tail_idx, rel_idx, neg_idx, edge_mask))

        piece = -(-(rel_rows * 25 // 8) // 64) * 8

        def away(bits):
            return [(sender, sender ^ bits) for sender in range(ent_devs)]

        def ring(step):
            shift = step + 1
            to_owner = [(sender, (sender + shift) % ent_devs) for sender in range(ent_devs)]
            return to_owner, [(target, sender) for sender, target in to_owner]

        asked = jnp.stack([tail_idx, neg_idx, rel_idx, edge_mask], axis=1)
        served = jnp.stack([lax.ppermute(asked[step], 'ent', ring(step)[0]) for step in range(rounds)])
        rows_all = jnp.concatenate([head_idx, served[:, 0], served[:, 1]], axis=1)
        keys = lax.sort(rows_all * 4096 + jnp.arange(3 * edges, dtype=jnp.int32)[None, :], dimension=1, is_stable=False)
        rel_keys = lax.sort(rel_idx * 1024 + jnp.arange(edges, dtype=jnp.int32)[None, :], dimension=1, is_stable=False)
        own_weight = jnp.pad(edge_mask.astype(F32), ((0, 8 - rounds), (0, 0))).T
        serve_weight = served[:, 3].astype(F32).reshape(rounds, edges // 256, 256)
        small = []
        for step in range(rounds):
            small.append((head_idx[step], served[step, 0], served[step, 1], served[step, 2], rel_idx[step], keys[step], rel_keys[step], serve_weight[step]))
        small, own_weight, rel_cols, ent_cols, ada_row = lax.optimization_barrier((small, own_weight, rel_table.T, ent_part.T, ada_part.reshape(1, part_rows)))

        cols = 512
        grad_rows = 2 * edges + max(edges, rel_rows)
        areas = {'grad': (part_rows, grad_rows), 'rel': (part_rows + grad_rows, rel_rows), 'drel': (part_rows + grad_rows + rel_rows, 2 * piece)}
        areas['loss'] = (sum(areas['drel']), rounds)
        tab_shape = pltpu.VMEM((sum(areas['loss']), 4, LANES), F32)
        head_wire, tail_wire = shape(edges * 25 // 16, LANES), shape(2 * edges * 25 // 8, LANES, dtype=BF16)
        part_wire, half_wire = shape(piece, LANES), shape(4 * piece, LANES)
        hold = pltpu.VMEM((edges, 4, LANES), F32)
        work = [pltpu.VMEM((edges, 512), F32), pltpu.VMEM((edges, 512), BF16)]

        def call(kernel, tab, inputs, in_specs, out_shape, out_specs, scratch=(), **more):
            ins, outs = len(inputs), len(out_shape)

            def body(*refs):
                kernel(*refs[:ins], *refs[ins + 2:ins + 2 + outs], refs[ins + 1], *refs[ins + 2 + outs:], areas=areas, **more)

            got = pl.pallas_call(
                body, in_specs=in_specs + [VM], out_specs=[VM] + out_specs, out_shape=[tab_shape] + out_shape,
                input_output_aliases={ins: 0}, scratch_shapes=list(scratch), compiler_params=params(GRANT))(*inputs, tab)
            return got[0], got[1:]

        tab = pl.pallas_call(
            load_kernel, in_specs=[HBM], out_specs=VM, out_shape=tab_shape,
            scratch_shapes=[pltpu.VMEM((4, DIM, cols), F32), pltpu.SemaphoreType.DMA((4,))],
            compiler_params=params(GRANT), name="load")(ent_cols)
        tab, _ = call(load_rel_kernel, tab, [rel_cols, ada_row], [VM, VM], [], [])
        half = None
        for step in range(rounds):
            to_owner, to_asker = ring(step)
            head_ids, serve_tails, serve_negs, serve_rel, own_rel, key, rel_key, weight = small[step]
            tab, (tails,) = call(gather_tails_kernel, tab, [serve_tails, serve_negs], [SM] * 2, [tail_wire], [VM], [hold])
            far_tails = lax.ppermute(tails, 'ent', to_asker)
            tab, heads = call(gather_heads_kernel, tab, [head_ids], [SM], [head_wire] * 2, [VM] * 2, [hold])
            if TAILS_FIRST[step % len(TAILS_FIRST)]:
                far_tails, *heads = lax.optimization_barrier((far_tails, *heads))
            far_heads = []
            for side in range(2):
                far_heads.append(lax.ppermute(heads[side], 'ent', to_owner))
            if step:
                tab, _ = call(rel_kernel, tab, [half, far_half], [VM] * 2, [], [])

            def tail_role(tab, side, last):
                return call(
                    tail_kernel, tab, [serve_rel, weight, far_heads[side], tails], [SM, VM, VM, VM], [], [],
                    [pltpu.VMEM((edges // 2, 512), F32), pltpu.VMEM((edges, 512), BF16), pltpu.VMEM((edges, 512), F32)], side=side, last=last)[0]

            tab, (give,) = call(
                head_kernel, tab, [own_rel, rel_key, own_weight, *heads, far_tails], [SM, SM, VM, VM, VM, VM],
                [half_wire], [VM], work, step_no=step)
            got = lax.ppermute(give, 'ent', away(1))
            tab, (own, *parts) = call(split_kernel, tab, [got], [VM], [part_wire] * 4, [VM] * 4)
            parts = [lax.ppermute(x, 'ent', away(2 * hop + 2)) for hop, x in enumerate(parts)]
            tab = tail_role(tab, 0, False)
            tab = tail_role(tab, 1, True)
            tab, (total,) = call(sum_kernel, tab, [own, *parts], [VM] * 4, [part_wire], [VM])
            totals = [lax.ppermute(total, 'ent', away(2 * hop + 2)) for hop in range(3)]
            tab, _ = call(update_kernel, tab, [key], [SM], [], [], [hold, hold])
            tab, (half,) = call(join_kernel, tab, [total, *totals], [VM] * 4, [half_wire], [VM])
            far_half = lax.ppermute(half, 'ent', away(1))
        tab, _ = call(rel_kernel, tab, [half, far_half], [VM] * 2, [], [])

        ent_out, ada_out = pl.pallas_call(
            store_kernel, grid=(part_rows // cols,), in_specs=[VM],
            out_specs=[pl.BlockSpec((DIM, cols), lambda i: (0, i)), pl.BlockSpec((1, cols), lambda i: (0, i))],
            out_shape=[shape(DIM, part_rows), shape(1, part_rows)], compiler_params=params(GRANT), name="store")(tab)
        rel_out, loss_out = pl.pallas_call(
            functools.partial(store_rel_kernel, areas=areas, edges=edges), in_specs=[VM], out_specs=[VM, VM],
            out_shape=[shape(DIM, rel_count), shape(1, LANES)], compiler_params=params(GRANT), name="store_rel")(tab)
        ent_out, ada_out, rel_out, loss_out = lax.optimization_barrier((ent_out, ada_out, rel_out, loss_out))
        return ent_out.T, ada_out.reshape(part_rows), rel_out.T, loss_out[:, :rounds]

    return jax.shard_map(train, mesh=mesh, in_specs=(row_spec, state_spec, rel_spec, edge_spec, edge_spec, edge_spec, edge_spec, edge_spec), out_specs=(row_spec, state_spec, rel_spec, row_spec), check_vma=False)
```

```python
import functools

import jax
import jax.numpy as jnp
from jax import lax
from jax.experimental import pallas as pl
from jax.experimental.pallas import tpu as pltpu
from jax.sharding import PartitionSpec as P


LEARN_RATE = 0.25
ADA_EPS = 1e-10

DIM = 400
HALF = 200
ACC_LANE = 16
LANES = 128
MIB = 1 << 20
GRANT = 7
TAILS_FIRST = (True, False)

VM = pl.BlockSpec(memory_space=pltpu.VMEM)
SM = pl.BlockSpec(memory_space=pltpu.SMEM)
HBM = pl.BlockSpec(memory_space=pltpu.HBM)
F32 = jnp.float32
BF16 = jnp.bfloat16


def params(mib):
    return pltpu.CompilerParams(vmem_limit_bytes=int(mib * MIB))


def lane_ids(shape):
    return lax.broadcasted_iota(jnp.int32, shape, 1)


def swap_two(x):
    return pltpu.roll(x, 64, 1)


def swap_three(x):
    return jnp.where(lane_ids(x.shape) < 8, pltpu.roll(x, 120, 1), pltpu.roll(x, 8, 1))


def times(a, b):
    out = [a[0] * b[0] - a[1] * b[1], a[0] * b[1] + a[1] * b[0]]
    for x, y, swap, edge in ((a[2], b[2], swap_two, 64), (a[3], b[3], swap_three, 8)):
        xs, ys = swap(x), swap(y)
        out.append(jnp.where(lane_ids(x.shape) < edge, x * y - xs * ys, xs * y + x * ys))
    return out


def times_conj(a, b):
    out = [a[0] * b[0] + a[1] * b[1], a[1] * b[0] - a[0] * b[1]]
    for x, y, swap, edge in ((a[2], b[2], swap_two, 64), (a[3], b[3], swap_three, 8)):
        xs, ys = swap(x), swap(y)
        out.append(jnp.where(lane_ids(x.shape) < edge, x * y + xs * ys, x * ys - xs * y))
    return out


def keep_data(x):
    return jnp.where(lane_ids(x.shape) < ACC_LANE, x, 0.0)


def flat(ref):
    return ref.reshape(ref.shape[0] * 4, LANES)


def plane(ref2, start, rows, part):
    return ref2[pl.ds(start * 4 + part, rows, stride=4), :]


def put_plane(ref2, start, rows, part, x):
    ref2[pl.ds(start * 4 + part, rows, stride=4), :] = x


def each(count, body, carry=0, base=0, unroll=16):
    def step(b, carry):
        at = b * unroll
        for u in range(unroll):
            carry = body(base + at, at, u, carry)
        return carry

    return lax.fori_loop(0, count // unroll, step, carry)


def copy_rows(idx_ref, count, src, dst, skip=0):
    def body(base, at, u, carry):
        dst[at + u] = src[idx_ref[base + (skip + u)]]
        return carry

    each(count, body)


def pack_rows(dst, src2, rows, first, groups, packed):
    step = rows // 8
    for g in range(groups):
        at, to = g * step, (first + g) * step
        for part in range(3):
            dst[part * rows + to:part * rows + to + step, :] = plane(src2, at, step, part).astype(dst.dtype)
        last = keep_data(plane(src2, at, step, 3))
        if first + g:
            last = pltpu.roll(last, 16 * (first + g), 1)
        packed = last if packed is None else packed + last
    if first + groups == 8:
        dst[3 * rows:3 * rows + step, :] = packed.astype(dst.dtype)
    return packed


def unpack_part(src, rows, g, step):
    planes = [src[part * rows + g * step:part * rows + (g + 1) * step, :].astype(F32) for part in range(3)]
    last = src[3 * rows:3 * rows + step, :].astype(F32)
    if g:
        last = pltpu.roll(last, LANES - 16 * g, 1)
    planes.append(keep_data(last))
    return planes


def row_parts(ent_ref, state, cols):
    return [
        ent_ref[0:128, :],
        ent_ref[HALF:HALF + 128, :],
        jnp.concatenate([ent_ref[128:192, :], ent_ref[HALF + 128:HALF + 192, :]], axis=0),
        jnp.concatenate([ent_ref[192:200, :], ent_ref[HALF + 192:HALF + 200, :], state, jnp.zeros((104, cols), F32)], axis=0),
    ]


def put_columns(ent_ref, x, part):
    if part < 2:
        ent_ref[part * HALF:part * HALF + 128, :] = x
    elif part == 2:
        ent_ref[128:192, :] = x[0:64]
        ent_ref[HALF + 128:HALF + 192, :] = x[64:128]
    else:
        ent_ref[192:200, :] = x[0:8]
        ent_ref[HALF + 192:HALF + 200, :] = x[8:16]


def load_kernel(ent_hbm, tab_ref, hold_ref, sems):
    cols = hold_ref.shape[2]
    blocks = ent_hbm.shape[1] // cols
    tab2 = flat(tab_ref)

    def fetch(b, slot):
        return pltpu.make_async_copy(ent_hbm.at[:, pl.ds(pl.multiple_of(b * cols, cols), cols)], hold_ref.at[slot], sems.at[slot])

    slots = hold_ref.shape[0]
    for b in range(slots - 1):
        fetch(b, b).start()

    def body(b, carry):
        slot = lax.rem(b, slots)
        fetch(b, slot).wait()
        ahead = b + slots - 1

        @pl.when(ahead < blocks)
        def _():
            fetch(ahead, lax.rem(ahead, slots)).start()

        parts = row_parts(hold_ref.at[slot], jnp.zeros((8, cols), F32), cols)
        for part in range(4):
            tab2[pl.ds(b * (cols * 4) + part, cols, stride=4), :] = parts[part].T
        return carry

    lax.fori_loop(0, blocks, body, 0)


def load_rel_kernel(rel_ref, ada_ref, tab_ref, *, areas):
    tab2 = flat(tab_ref)
    block = 512

    def body(b, carry):
        state = jnp.broadcast_to(ada_ref[:, pl.ds(pl.multiple_of(b * block, block), block)], (LANES, block)).T
        at = pl.ds(b * (block * 4) + 3, block, stride=4)
        tab2[at, :] = jnp.where(lane_ids(state.shape) == ACC_LANE, state, tab2[at, :])
        return carry

    lax.fori_loop(0, ada_ref.shape[1] // block, body, 0)
    base, rows = areas['rel']
    count = rel_ref.shape[1]
    parts = row_parts(rel_ref, jnp.zeros((8, count), F32), count)
    for part in range(4):
        tab2[pl.ds(4 * base + part, count, stride=4), :] = parts[part].T
    tab_ref[base + count:base + rows] = jnp.zeros((rows - count, 4, LANES), F32)


def store_kernel(tab_ref, ent_ref, ada_ref):
    cols = ent_ref.shape[1]
    tab2 = flat(tab_ref)
    start = pl.program_id(0) * (cols * 4)
    for part in range(4):
        x = tab2[pl.ds(start + part, cols, stride=4), :].T
        put_columns(ent_ref, x, part)
        if part == 3:
            ada_ref[...] = x[ACC_LANE:ACC_LANE + 1]


def store_rel_kernel(tab_ref, rel_ref, loss_ref, *, areas, edges):
    tab2 = flat(tab_ref)
    count = rel_ref.shape[1]
    for part in range(4):
        put_columns(rel_ref, tab2[pl.ds(4 * areas['rel'][0] + part, count, stride=4), :].T, part)
    base, rounds = areas['loss']
    lane = lane_ids((1, LANES))
    total = jnp.zeros((1, LANES), F32)
    for step in range(rounds):
        total = jnp.where(lane == step, tab2[4 * (base + step):4 * (base + step) + 1, :], total)
    loss_ref[...] = total * (1.0 / edges)


def gather_tails_kernel(tail_ref, neg_ref, tail_out, tab_ref, hold_ref, *, areas):
    edges = tail_ref.shape[0]
    hold2 = flat(hold_ref)
    copy_rows(tail_ref, edges, tab_ref, hold_ref)
    packed = pack_rows(tail_out, hold2, 2 * edges, 0, 4, None)
    copy_rows(neg_ref, edges, tab_ref, hold_ref)
    pack_rows(tail_out, hold2, 2 * edges, 4, 4, packed)


def gather_heads_kernel(head_ref, one_out, two_out, tab_ref, hold_ref, *, areas):
    edges = head_ref.shape[0]
    copy_rows(head_ref, edges, tab_ref, hold_ref)
    for side, out in enumerate((one_out, two_out)):
        half = hold_ref.at[pl.ds(side * (edges // 2), edges // 2)]
        pack_rows(out, flat(half), edges // 2, 0, 8, None)


def adagrad(grad, row):
    total = grad[0] * grad[0] + grad[1] * grad[1] + grad[2] * grad[2] + grad[3] * grad[3]
    mean = jnp.sum(total, axis=1, keepdims=True) * (1.0 / DIM)
    lane = lane_ids(row[3].shape)
    state = jnp.sum(jnp.where(lane == ACC_LANE, row[3], 0.0), axis=1, keepdims=True) + mean
    rate = LEARN_RATE / jnp.sqrt(state + ADA_EPS)
    new = [row[part] - grad[part] * rate for part in range(4)]
    new[3] = jnp.where(lane == ACC_LANE, state, new[3])
    return new


def apply_rows(plan_ref, same_ref, grad_ref, tab_ref, sum_ref, row_ref):
    size = sum_ref.shape[0]
    count = same_ref.shape[0]
    sum2, row2 = flat(sum_ref), flat(row_ref)
    block = 128

    def chunk(c, acc):
        base = c * size

        def collect(base, at, u, acc):
            acc = acc * same_ref[base + u] + grad_ref[plan_ref[base + u]]
            sum_ref[at + u] = acc
            row_ref[at + u] = tab_ref[plan_ref[base + (count + u)]]
            return acc

        acc = each(size, collect, acc, base)

        def update(b, carry):
            at = b * (block * 4)
            grad = [sum2[pl.ds(at + part, block, stride=4), :] for part in range(4)]
            row = [row2[pl.ds(at + part, block, stride=4), :] for part in range(4)]
            new = adagrad(grad, row)
            for part in range(4):
                row2[pl.ds(at + part, block, stride=4), :] = new[part]
            return carry

        lax.fori_loop(0, size // block, update, 0)

        def write(base, at, u, carry):
            tab_ref[plan_ref[base + (2 * count + u)]] = row_ref[at + u]
            return carry

        each(size, write, 0, base)
        return acc

    lax.fori_loop(0, count // size, chunk, jnp.zeros((4, LANES), F32))


def update_kernel(plan_ref, same_ref, tab_ref, sum_ref, row_ref, *, areas):
    apply_rows(plan_ref, same_ref, tab_ref.at[pl.ds(*areas['grad'])], tab_ref, sum_ref, row_ref)


def put_wide(ref, start, rows, planes):
    for part in range(4):
        ref[start:start + rows, part * LANES:(part + 1) * LANES] = planes[part].astype(ref.dtype)


def unpack_negs(tail_ref, neg_ref):
    edges = neg_ref.shape[0]
    wide = edges // 4
    for g in range(4):
        put_wide(neg_ref, g * wide, wide, unpack_part(tail_ref, 2 * edges, g + 4, wide))


def put_queries(head_ref, hold2, query_ref, start):
    rows = head_ref.shape[0] * 8 // 25
    step = rows // 8
    for g in range(8):
        heads = unpack_part(head_ref, rows, g, step)
        rels = [plane(hold2, start + g * step, step, part) for part in range(4)]
        rels[3] = keep_data(rels[3])
        put_wide(query_ref, start + g * step, step, times(heads, rels))


def tail_block(tail_ref, b, block):
    rows = 8 * block
    planes = [tail_ref[pl.ds(pl.multiple_of(part * rows + b * block, block), block), :].astype(F32) for part in range(3)]
    last = tail_ref[3 * rows:3 * rows + block, :].astype(F32)
    planes.append(keep_data(pltpu.roll(last, LANES - 16 * b, 1)))
    return planes


def head_kernel(rel_ref, plan_ref, same_ref, weight_ref, one_ref, two_ref, tail_ref, give_out, tab_ref, query_ref, neg_ref, *, areas, step_no):
    rel_tab, grad_out = tab_ref.at[pl.ds(*areas['rel'])], tab_ref.at[pl.ds(*areas['grad'])]
    edges = rel_ref.shape[0]
    hold_ref = grad_out.at[pl.ds(edges, edges)]
    copy_rows(rel_ref, edges, rel_tab, hold_ref)
    unpack_negs(tail_ref, neg_ref)
    scale = DIM ** -0.5
    for side, head_ref in enumerate((one_ref, two_ref)):
        put_queries(head_ref, flat(hold_ref), query_ref, side * (edges // 2))
    block = edges // 4

    def body(b, loss):
        at = pl.ds(pl.multiple_of(b * block, block), block)
        query = query_ref[at, :]
        tails = jnp.concatenate(tail_block(tail_ref, b, block), axis=1)
        pos = scale * jnp.sum(query * tails, axis=1, keepdims=True)
        neg = scale * lax.dot_general(query.astype(BF16), neg_ref[...], (((1,), (1,)), ((), ())), preferred_element_type=F32)
        top = jnp.maximum(pos, jnp.max(neg, axis=1, keepdims=True))
        pos_exp = jnp.exp(pos - top)
        neg_exp = jnp.exp(neg - top)
        denom = pos_exp + jnp.sum(neg_exp, axis=1, keepdims=True)
        weight = weight_ref[at, step_no:step_no + 1]
        loss = loss + weight * (top + jnp.log(denom) - pos)
        d_pos = weight * (pos_exp / denom - 1.0)
        d_neg = ((weight / denom) * neg_exp).astype(BF16)
        query_ref[at, :] = scale * (d_pos * tails + jnp.dot(d_neg, neg_ref[...], preferred_element_type=F32))
        return loss

    loss = lax.fori_loop(0, edges // block, body, jnp.zeros((block, 1), F32))
    tab_ref[areas['loss'][0] + step_no] = jnp.broadcast_to(jnp.sum(loss, axis=0, keepdims=True), (4, LANES))
    hold2, grad2 = flat(hold_ref), flat(grad_out)
    half = edges // 2
    step = half // 8
    for side, head_ref in enumerate((one_ref, two_ref)):
        for g in range(8):
            at = side * half + g * step
            heads = unpack_part(head_ref, half, g, step)
            rels = [plane(hold2, at, step, part) for part in range(4)]
            rels[3] = keep_data(rels[3])
            d_query = [query_ref[at:at + step, part * LANES:(part + 1) * LANES] for part in range(4)]
            d_head = times_conj(d_query, rels)
            d_rel = times_conj(d_query, heads)
            for part in range(4):
                put_plane(grad2, at, step, part, d_head[part])
                put_plane(hold2, at, step, part, d_rel[part])

    rel_rows = rel_tab.shape[0]
    sum_ref = grad_out.at[pl.ds(2 * edges, rel_rows)]
    sum_ref[...] = jnp.zeros(sum_ref.shape, F32)

    def scatter(base, at, u, acc):
        acc = acc * same_ref[base + u] + hold_ref[plan_ref[base + u]]
        sum_ref[plan_ref[base + (edges + u)]] = acc
        return acc

    each(edges, scatter, jnp.zeros((4, LANES), F32))
    drel_out = flat(tab_ref.at[pl.ds(*areas['drel'])])
    pack_rows(drel_out, flat(sum_ref), rel_rows, 0, 8, None)
    used, half = rel_rows * 25 // 8, give_out.shape[0]
    drel_out[used:, :] = jnp.zeros((2 * half - used, LANES), F32)
    core = lax.rem(lax.axis_index('ent'), 2)
    give_out[...] = drel_out[pl.ds(pl.multiple_of((1 - core) * half, 8), half), :]


def tail_kernel(rel_ref, weight_ref, head_ref, tail_ref, tab_ref, query_ref, neg_ref, sum_ref, *, areas, side, last):
    rel_tab, grad_out = tab_ref.at[pl.ds(*areas['rel'])], tab_ref.at[pl.ds(*areas['grad'])]
    edges = neg_ref.shape[0]
    half = edges // 2
    hold_ref = grad_out.at[pl.ds(edges + side * half, half)]
    unpack_negs(tail_ref, neg_ref)

    copy_rows(rel_ref, half, rel_tab, hold_ref, side * half)
    put_queries(head_ref, flat(hold_ref), query_ref, 0)
    scale = DIM ** -0.5
    block = edges // 4
    grad2 = flat(grad_out)
    sum_ref[...] = jnp.zeros(sum_ref.shape, F32)

    def body(b, carry):
        at = pl.ds(pl.multiple_of(b * block, block), block)
        query = query_ref[at, :]
        query_bf = query.astype(BF16)
        tails = tail_block(tail_ref, b + 2 * side, block)
        prod = [query[:, part * LANES:(part + 1) * LANES] * tails[part] for part in range(4)]
        prod = (prod[0] + prod[1]) + (prod[2] + prod[3])
        pos = scale * jnp.sum(prod.T, axis=0, keepdims=True)
        neg = scale * lax.dot_general(neg_ref[...], query_bf, (((1,), (1,)), ((), ())), preferred_element_type=F32)
        top = jnp.maximum(pos, jnp.max(neg, axis=0, keepdims=True))
        pos_exp = jnp.exp(pos - top)
        neg_exp = jnp.exp(neg - top)
        denom = pos_exp + jnp.sum(neg_exp, axis=0, keepdims=True)
        weight = weight_ref[pl.ds(b + 2 * side, 1), :]
        d_pos = weight * (pos_exp / denom - 1.0)
        d_neg = ((weight / denom) * neg_exp).astype(BF16)
        sum_ref[...] += jnp.dot(d_neg, query_bf, preferred_element_type=F32)
        d_pos_col = jnp.broadcast_to(d_pos, (LANES, block)).T
        for part in range(4):
            grad2[pl.ds((edges + side * half + b * block) * 4 + part, block, stride=4), :] = scale * d_pos_col * query[:, part * LANES:(part + 1) * LANES]
        return carry

    lax.fori_loop(0, half // block, body, 0)
    for part in range(4):
        total = scale * sum_ref[:, part * LANES:(part + 1) * LANES]
        if last:
            total = total + plane(grad2, 2 * edges, edges, part)
        put_plane(grad2, 2 * edges, edges, part, total)


def split_kernel(got_ref, own_out, one_out, two_out, three_out, tab_ref, *, areas):
    drel_ref = flat(tab_ref.at[pl.ds(*areas['drel'])])
    half, piece = got_ref.shape[0], own_out.shape[0]
    me = lax.axis_index('ent')
    core, chip = lax.rem(me, 2), lax.div(me, 2)
    for away, out in enumerate((own_out, one_out, two_out, three_out)):
        at = pl.multiple_of((chip ^ away) * piece, 8)
        out[...] = drel_ref[pl.ds(pl.multiple_of(core * half + at, 8), piece), :] + got_ref[pl.ds(at, piece), :]


def sum_kernel(own_ref, one_ref, two_ref, three_ref, out, tab_ref, *, areas):
    out[...] = (own_ref[...] + one_ref[...]) + (two_ref[...] + three_ref[...])


def join_kernel(own_ref, one_ref, two_ref, three_ref, out, tab_ref, *, areas):
    piece = own_ref.shape[0]
    chip = lax.div(lax.axis_index('ent'), 2)
    for away, ref in enumerate((own_ref, one_ref, two_ref, three_ref)):
        out[pl.ds(pl.multiple_of((chip ^ away) * piece, 8), piece), :] = ref[...]


def rel_kernel(half_ref, far_ref, tab_ref, *, areas):
    drel_ref = flat(tab_ref.at[pl.ds(*areas['drel'])])
    rel_tab = tab_ref.at[pl.ds(*areas['rel'])]
    rows = rel_tab.shape[0]
    half = half_ref.shape[0]
    core = lax.rem(lax.axis_index('ent'), 2)
    drel_ref[pl.ds(pl.multiple_of(core * half, 8), half), :] = half_ref[...]
    drel_ref[pl.ds(pl.multiple_of((1 - core) * half, 8), half), :] = far_ref[...]
    step = rows // 8
    rel2 = flat(rel_tab)
    for g in range(8):
        grad = unpack_part(drel_ref, rows, g, step)
        row = [plane(rel2, g * step, step, part) for part in range(4)]
        new = adagrad(grad, row)
        for part in range(4):
            put_plane(rel2, g * step, step, part, new[part])


def shape(*dims, dtype=F32):
    return jax.ShapeDtypeStruct(dims, dtype)


def solution(mesh):
    ent_devs = mesh.shape['ent']
    row_spec = P(('sweep', 'ent'), None)
    state_spec = P(('sweep', 'ent'))
    rel_spec = P('sweep', None)
    edge_spec = P(('sweep', 'ent'), None, None)

    def train(ent_part, ada_part, rel_table, head_idx, tail_idx, rel_idx, neg_idx, edge_mask):
        part_rows = ent_part.shape[0]
        rel_count = rel_table.shape[0]
        rounds = head_idx.shape[1]
        edges = head_idx.shape[2]
        rel_rows = -(-rel_count // 128) * 128
        piece = -(-(rel_rows * 25 // 8) // 64) * 8
        head_idx, tail_idx, rel_idx, neg_idx, edge_mask = (x[0] for x in (head_idx, tail_idx, rel_idx, neg_idx, edge_mask))


        def away(bits):
            return [(sender, sender ^ bits) for sender in range(ent_devs)]

        def ring(step):
            shift = step + 1
            to_owner = [(sender, (sender + shift) % ent_devs) for sender in range(ent_devs)]
            return to_owner, [(target, sender) for sender, target in to_owner]

        asked = jnp.stack([tail_idx, neg_idx, rel_idx, edge_mask], axis=1)
        served = jnp.stack([lax.ppermute(asked[step], 'ent', ring(step)[0]) for step in range(rounds)])
        rows_all = jnp.concatenate([head_idx, served[:, 0], served[:, 1]], axis=1)
        keys = lax.sort(rows_all * 4096 + jnp.arange(3 * edges, dtype=jnp.int32)[None, :], dimension=1, is_stable=False)
        rel_keys = lax.sort(rel_idx * 1024 + jnp.arange(edges, dtype=jnp.int32)[None, :], dimension=1, is_stable=False)
        own_weight = jnp.pad(edge_mask.astype(F32), ((0, 8 - rounds), (0, 0))).T
        serve_weight = served[:, 3].astype(F32).reshape(rounds, edges // 256, 256)

        def plan(keys, bits, spare):
            rows, places = keys >> bits, keys & ((1 << bits) - 1)
            equal = rows[:, 1:] == rows[:, :-1]
            no = jnp.zeros((rounds, 1), jnp.bool_)
            parts = [places, rows]
            if spare is not None:
                parts.append(jnp.where(jnp.concatenate([equal, no], axis=1), spare, rows))
            return jnp.concatenate(parts, axis=1), jnp.concatenate([no, equal], axis=1).astype(F32)

        total_rows = part_rows + 2 * edges + max(edges, rel_rows) + rel_rows + 2 * piece + rounds
        moves, same = plan(keys, 12, total_rows)
        rel_moves, rel_same = plan(rel_keys, 10, None)
        small = []
        for step in range(rounds):
            small.append((head_idx[step], served[step, 0], served[step, 1], served[step, 2], rel_idx[step], moves[step], same[step], rel_moves[step], rel_same[step], serve_weight[step]))
        small, own_weight, rel_cols, ent_cols, ada_row = lax.optimization_barrier((small, own_weight, rel_table.T, ent_part.T, ada_part.reshape(1, part_rows)))

        cols = 512
        grad_rows = 2 * edges + max(edges, rel_rows)
        areas = {'grad': (part_rows, grad_rows), 'rel': (part_rows + grad_rows, rel_rows), 'drel': (part_rows + grad_rows + rel_rows, 2 * piece)}
        areas['loss'] = (sum(areas['drel']), rounds)
        tab_shape = pltpu.VMEM((total_rows + 2, 4, LANES), F32)
        head_wire, tail_wire = shape(edges * 25 // 16, LANES), shape(2 * edges * 25 // 8, LANES, dtype=BF16)
        part_wire, half_wire = shape(piece, LANES), shape(4 * piece, LANES)
        hold = pltpu.VMEM((edges, 4, LANES), F32)
        work = [pltpu.VMEM((edges, 512), F32), pltpu.VMEM((edges, 512), BF16)]

        def call(kernel, tab, inputs, in_specs, out_shape, out_specs, scratch=(), **more):
            ins, outs = len(inputs), len(out_shape)

            def body(*refs):
                kernel(*refs[:ins], *refs[ins + 2:ins + 2 + outs], refs[ins + 1], *refs[ins + 2 + outs:], areas=areas, **more)

            got = pl.pallas_call(
                body, in_specs=in_specs + [VM], out_specs=[VM] + out_specs, out_shape=[tab_shape] + out_shape,
                input_output_aliases={ins: 0}, scratch_shapes=list(scratch), compiler_params=params(GRANT))(*inputs, tab)
            return got[0], got[1:]

        tab = pl.pallas_call(
            load_kernel, in_specs=[HBM], out_specs=VM, out_shape=tab_shape,
            scratch_shapes=[pltpu.VMEM((4, DIM, cols), F32), pltpu.SemaphoreType.DMA((4,))],
            compiler_params=params(GRANT), name="load")(ent_cols)
        tab, _ = call(load_rel_kernel, tab, [rel_cols, ada_row], [VM, VM], [], [])
        half = None
        for step in range(rounds):
            to_owner, to_asker = ring(step)
            head_ids, serve_tails, serve_negs, serve_rel, own_rel, move, equal, rel_move, rel_equal, weight = small[step]
            tab, (tails,) = call(gather_tails_kernel, tab, [serve_tails, serve_negs], [SM] * 2, [tail_wire], [VM], [hold])
            far_tails = lax.ppermute(tails, 'ent', to_asker)
            tab, heads = call(gather_heads_kernel, tab, [head_ids], [SM], [head_wire] * 2, [VM] * 2, [hold])
            if TAILS_FIRST[step % len(TAILS_FIRST)]:
                far_tails, *heads = lax.optimization_barrier((far_tails, *heads))
            far_heads = []
            for side in range(2):
                far_heads.append(lax.ppermute(heads[side], 'ent', to_owner))
            if step:
                tab, _ = call(rel_kernel, tab, [half, far_half], [VM] * 2, [], [])

            def tail_role(tab, side, last):
                return call(
                    tail_kernel, tab, [serve_rel, weight, far_heads[side], tails], [SM, VM, VM, VM], [], [],
                    [pltpu.VMEM((edges // 2, 512), F32), pltpu.VMEM((edges, 512), BF16), pltpu.VMEM((edges, 512), F32)], side=side, last=last)[0]

            tab, (give,) = call(
                head_kernel, tab, [own_rel, rel_move, rel_equal, own_weight, *heads, far_tails], [SM] * 3 + [VM] * 4,
                [half_wire], [VM], work, step_no=step)
            got = lax.ppermute(give, 'ent', away(1))
            tab, (own, *parts) = call(split_kernel, tab, [got], [VM], [part_wire] * 4, [VM] * 4)
            parts = [lax.ppermute(x, 'ent', away(2 * hop + 2)) for hop, x in enumerate(parts)]
            tab = tail_role(tab, 0, False)
            tab = tail_role(tab, 1, True)
            tab, (total,) = call(sum_kernel, tab, [own, *parts], [VM] * 4, [part_wire], [VM])
            totals = [lax.ppermute(total, 'ent', away(2 * hop + 2)) for hop in range(3)]
            tab, _ = call(update_kernel, tab, [move, equal], [SM] * 2, [], [], [hold, hold])
            tab, (half,) = call(join_kernel, tab, [total, *totals], [VM] * 4, [half_wire], [VM])
            far_half = lax.ppermute(half, 'ent', away(1))
        tab, _ = call(rel_kernel, tab, [half, far_half], [VM] * 2, [], [])

        ent_out, ada_out = pl.pallas_call(
            store_kernel, grid=(part_rows // cols,), in_specs=[VM],
            out_specs=[pl.BlockSpec((DIM, cols), lambda i: (0, i)), pl.BlockSpec((1, cols), lambda i: (0, i))],
            out_shape=[shape(DIM, part_rows), shape(1, part_rows)], compiler_params=params(GRANT), name="store")(tab)
        rel_out, loss_out = pl.pallas_call(
            functools.partial(store_rel_kernel, areas=areas, edges=edges), in_specs=[VM], out_specs=[VM, VM],
            out_shape=[shape(DIM, rel_count), shape(1, LANES)], compiler_params=params(GRANT), name="store_rel")(tab)
        ent_out, ada_out, rel_out, loss_out = lax.optimization_barrier((ent_out, ada_out, rel_out, loss_out))
        return ent_out.T, ada_out.reshape(part_rows), rel_out.T, loss_out[:, :rounds]

    return jax.shard_map(train, mesh=mesh, in_specs=(row_spec, state_spec, rel_spec, edge_spec, edge_spec, edge_spec, edge_spec, edge_spec), out_specs=(row_spec, state_spec, rel_spec, row_spec), check_vma=False)
```

```python
import functools

import jax
import jax.numpy as jnp
from jax import lax
from jax.experimental import pallas as pl
from jax.experimental.pallas import tpu as pltpu
from jax.sharding import PartitionSpec as P


LEARN_RATE = 0.25
ADA_EPS = 1e-10

DIM = 400
HALF = 200
ACC_LANE = 16
LANES = 128
MIB = 1 << 20
GRANT = 7
STEP = 16
TAILS_FIRST = (True, False)

VM = pl.BlockSpec(memory_space=pltpu.VMEM)
SM = pl.BlockSpec(memory_space=pltpu.SMEM)
HBM = pl.BlockSpec(memory_space=pltpu.HBM)
F32 = jnp.float32
BF16 = jnp.bfloat16


def params(mib):
    return pltpu.CompilerParams(vmem_limit_bytes=int(mib * MIB))


def lane_ids(shape):
    return lax.broadcasted_iota(jnp.int32, shape, 1)


def swap_two(x):
    return pltpu.roll(x, 64, 1)


def swap_three(x):
    return jnp.where(lane_ids(x.shape) < 8, pltpu.roll(x, 120, 1), pltpu.roll(x, 8, 1))


def times(a, b):
    out = [a[0] * b[0] - a[1] * b[1], a[0] * b[1] + a[1] * b[0]]
    for x, y, swap, edge in ((a[2], b[2], swap_two, 64), (a[3], b[3], swap_three, 8)):
        xs, ys = swap(x), swap(y)
        out.append(jnp.where(lane_ids(x.shape) < edge, x * y - xs * ys, xs * y + x * ys))
    return out


def times_conj(a, b):
    out = [a[0] * b[0] + a[1] * b[1], a[1] * b[0] - a[0] * b[1]]
    for x, y, swap, edge in ((a[2], b[2], swap_two, 64), (a[3], b[3], swap_three, 8)):
        xs, ys = swap(x), swap(y)
        out.append(jnp.where(lane_ids(x.shape) < edge, x * y + xs * ys, x * ys - xs * y))
    return out


def keep_data(x):
    return jnp.where(lane_ids(x.shape) < ACC_LANE, x, 0.0)


def flat(ref):
    return ref.reshape(ref.shape[0] * 4, LANES)


def plane(ref2, start, rows, part):
    return ref2[pl.ds(start * 4 + part, rows, stride=4), :]


def put_plane(ref2, start, rows, part, x):
    ref2[pl.ds(start * 4 + part, rows, stride=4), :] = x


def each(count, body, carry=0, base=0, unroll=16):
    def step(b, carry):
        at = b * unroll
        for u in range(unroll):
            carry = body(base + at, at, u, carry)
        return carry

    return lax.fori_loop(0, count // unroll, step, carry)


def run_sums(acc, grads, same):
    sums = []
    for u in range(0, len(grads), 2):
        first, second = same[u], same[u + 1]
        sums.append(acc * first + grads[u])
        both = jnp.full(acc.shape, first, F32) * second
        acc = acc * both + (grads[u] * second + grads[u + 1])
        sums.append(acc)
    return acc, sums


def copy_rows(idx_ref, count, src, dst, skip=0):
    def body(base, at, u, carry):
        dst[at + u] = src[idx_ref[base + (skip + u)]]
        return carry

    each(count, body)


def pack_rows(dst, src2, rows, first, groups, packed):
    step = rows // 8
    for g in range(groups):
        at, to = g * step, (first + g) * step
        for part in range(3):
            dst[part * rows + to:part * rows + to + step, :] = plane(src2, at, step, part).astype(dst.dtype)
        last = keep_data(plane(src2, at, step, 3))
        if first + g:
            last = pltpu.roll(last, 16 * (first + g), 1)
        packed = last if packed is None else packed + last
    if first + groups == 8:
        dst[3 * rows:3 * rows + step, :] = packed.astype(dst.dtype)
    return packed


def unpack_part(src, rows, g, step):
    planes = [src[part * rows + g * step:part * rows + (g + 1) * step, :].astype(F32) for part in range(3)]
    last = src[3 * rows:3 * rows + step, :].astype(F32)
    if g:
        last = pltpu.roll(last, LANES - 16 * g, 1)
    planes.append(keep_data(last))
    return planes


def row_parts(ent_ref, state, cols):
    return [
        ent_ref[0:128, :],
        ent_ref[HALF:HALF + 128, :],
        jnp.concatenate([ent_ref[128:192, :], ent_ref[HALF + 128:HALF + 192, :]], axis=0),
        jnp.concatenate([ent_ref[192:200, :], ent_ref[HALF + 192:HALF + 200, :], state, jnp.zeros((104, cols), F32)], axis=0),
    ]


def put_columns(ent_ref, x, part):
    if part < 2:
        ent_ref[part * HALF:part * HALF + 128, :] = x
    elif part == 2:
        ent_ref[128:192, :] = x[0:64]
        ent_ref[HALF + 128:HALF + 192, :] = x[64:128]
    else:
        ent_ref[192:200, :] = x[0:8]
        ent_ref[HALF + 192:HALF + 200, :] = x[8:16]


def load_kernel(ent_hbm, tab_ref, hold_ref, sems):
    cols = hold_ref.shape[2]
    blocks = ent_hbm.shape[1] // cols
    tab2 = flat(tab_ref)

    def fetch(b, slot):
        return pltpu.make_async_copy(ent_hbm.at[:, pl.ds(pl.multiple_of(b * cols, cols), cols)], hold_ref.at[slot], sems.at[slot])

    slots = hold_ref.shape[0]
    for b in range(slots - 1):
        fetch(b, b).start()

    def body(b, carry):
        slot = lax.rem(b, slots)
        fetch(b, slot).wait()
        ahead = b + slots - 1

        @pl.when(ahead < blocks)
        def _():
            fetch(ahead, lax.rem(ahead, slots)).start()

        parts = row_parts(hold_ref.at[slot], jnp.zeros((8, cols), F32), cols)
        for part in range(4):
            tab2[pl.ds(b * (cols * 4) + part, cols, stride=4), :] = parts[part].T
        return carry

    lax.fori_loop(0, blocks, body, 0)


def load_rel_kernel(rel_ref, ada_ref, tab_ref, *, areas):
    tab2 = flat(tab_ref)
    block = 512

    def body(b, carry):
        state = jnp.broadcast_to(ada_ref[:, pl.ds(pl.multiple_of(b * block, block), block)], (LANES, block)).T
        at = pl.ds(b * (block * 4) + 3, block, stride=4)
        tab2[at, :] = jnp.where(lane_ids(state.shape) == ACC_LANE, state, tab2[at, :])
        return carry

    lax.fori_loop(0, ada_ref.shape[1] // block, body, 0)
    base, rows = areas['rel']
    count = rel_ref.shape[1]
    parts = row_parts(rel_ref, jnp.zeros((8, count), F32), count)
    for part in range(4):
        tab2[pl.ds(4 * base + part, count, stride=4), :] = parts[part].T
    tab_ref[base + count:base + rows] = jnp.zeros((rows - count, 4, LANES), F32)


def store_kernel(tab_ref, ent_ref, ada_ref):
    cols = ent_ref.shape[1]
    tab2 = flat(tab_ref)
    start = pl.program_id(0) * (cols * 4)
    for part in range(4):
        x = tab2[pl.ds(start + part, cols, stride=4), :].T
        put_columns(ent_ref, x, part)
        if part == 3:
            ada_ref[...] = x[ACC_LANE:ACC_LANE + 1]


def store_rel_kernel(tab_ref, rel_ref, loss_ref, *, areas, edges):
    tab2 = flat(tab_ref)
    count = rel_ref.shape[1]
    for part in range(4):
        put_columns(rel_ref, tab2[pl.ds(4 * areas['rel'][0] + part, count, stride=4), :].T, part)
    base, rounds = areas['loss']
    lane = lane_ids((1, LANES))
    total = jnp.zeros((1, LANES), F32)
    for step in range(rounds):
        total = jnp.where(lane == step, tab2[4 * (base + step):4 * (base + step) + 1, :], total)
    loss_ref[...] = total * (1.0 / edges)


def gather_tails_kernel(tail_ref, neg_ref, tail_out, tab_ref, hold_ref, *, areas):
    edges = tail_ref.shape[0]
    hold2 = flat(hold_ref)
    copy_rows(tail_ref, edges, tab_ref, hold_ref)
    packed = pack_rows(tail_out, hold2, 2 * edges, 0, 4, None)
    copy_rows(neg_ref, edges, tab_ref, hold_ref)
    pack_rows(tail_out, hold2, 2 * edges, 4, 4, packed)


def gather_heads_kernel(head_ref, one_out, two_out, tab_ref, hold_ref, *, areas):
    edges = head_ref.shape[0]
    copy_rows(head_ref, edges, tab_ref, hold_ref)
    for side, out in enumerate((one_out, two_out)):
        half = hold_ref.at[pl.ds(side * (edges // 2), edges // 2)]
        pack_rows(out, flat(half), edges // 2, 0, 8, None)


def adagrad(grad, row):
    total = grad[0] * grad[0] + grad[1] * grad[1] + grad[2] * grad[2] + grad[3] * grad[3]
    mean = jnp.sum(total, axis=1, keepdims=True) * (1.0 / DIM)
    lane = lane_ids(row[3].shape)
    state = jnp.sum(jnp.where(lane == ACC_LANE, row[3], 0.0), axis=1, keepdims=True) + mean
    rate = LEARN_RATE / jnp.sqrt(state + ADA_EPS)
    new = [row[part] - grad[part] * rate for part in range(4)]
    new[3] = jnp.where(lane == ACC_LANE, state, new[3])
    return new


def apply_rows(plan_ref, same_ref, grad_ref, tab_ref, sum_ref, row_ref):
    size = sum_ref.shape[0]
    count = same_ref.shape[0]
    sum2, row2 = flat(sum_ref), flat(row_ref)
    block = 128

    def chunk(c, acc):
        base = c * size

        def collect(b, acc):
            at = b * STEP
            src = base + at
            grads = [grad_ref[plan_ref[src + u]] for u in range(STEP)]
            acc, sums = run_sums(acc, grads, [same_ref[src + u] for u in range(STEP)])
            for u in range(STEP):
                sum_ref[at + u] = sums[u]
                row_ref[at + u] = tab_ref[plan_ref[src + (count + u)]]
            return acc

        acc = lax.fori_loop(0, size // STEP, collect, acc)

        def update(b, carry):
            at = b * (block * 4)
            grad = [sum2[pl.ds(at + part, block, stride=4), :] for part in range(4)]
            row = [row2[pl.ds(at + part, block, stride=4), :] for part in range(4)]
            new = adagrad(grad, row)
            for part in range(4):
                row2[pl.ds(at + part, block, stride=4), :] = new[part]
            return carry

        lax.fori_loop(0, size // block, update, 0)

        def write(base, at, u, carry):
            tab_ref[plan_ref[base + (2 * count + u)]] = row_ref[at + u]
            return carry

        each(size, write, 0, base)
        return acc

    lax.fori_loop(0, count // size, chunk, jnp.zeros((4, LANES), F32))


def update_kernel(plan_ref, same_ref, tab_ref, sum_ref, row_ref, *, areas):
    apply_rows(plan_ref, same_ref, tab_ref.at[pl.ds(*areas['grad'])], tab_ref, sum_ref, row_ref)


def put_wide(ref, start, rows, planes):
    for part in range(4):
        ref[start:start + rows, part * LANES:(part + 1) * LANES] = planes[part].astype(ref.dtype)


def unpack_negs(tail_ref, neg_ref):
    edges = neg_ref.shape[0]
    wide = edges // 4
    for g in range(4):
        put_wide(neg_ref, g * wide, wide, unpack_part(tail_ref, 2 * edges, g + 4, wide))


def put_queries(head_ref, hold2, query_ref, start):
    rows = head_ref.shape[0] * 8 // 25
    step = rows // 8
    for g in range(8):
        heads = unpack_part(head_ref, rows, g, step)
        rels = [plane(hold2, start + g * step, step, part) for part in range(4)]
        rels[3] = keep_data(rels[3])
        put_wide(query_ref, start + g * step, step, times(heads, rels))


def tail_block(tail_ref, b, block):
    rows = 8 * block
    planes = [tail_ref[pl.ds(pl.multiple_of(part * rows + b * block, block), block), :].astype(F32) for part in range(3)]
    last = tail_ref[3 * rows:3 * rows + block, :].astype(F32)
    planes.append(keep_data(pltpu.roll(last, LANES - 16 * b, 1)))
    return planes


def head_kernel(rel_ref, plan_ref, same_ref, weight_ref, one_ref, two_ref, tail_ref, give_out, tab_ref, query_ref, neg_ref, *, areas, step_no):
    rel_tab, grad_out = tab_ref.at[pl.ds(*areas['rel'])], tab_ref.at[pl.ds(*areas['grad'])]
    edges = rel_ref.shape[0]
    hold_ref = grad_out.at[pl.ds(edges, edges)]
    copy_rows(rel_ref, edges, rel_tab, hold_ref)
    unpack_negs(tail_ref, neg_ref)
    scale = DIM ** -0.5
    for side, head_ref in enumerate((one_ref, two_ref)):
        put_queries(head_ref, flat(hold_ref), query_ref, side * (edges // 2))
    block = edges // 4

    def body(b, loss):
        at = pl.ds(pl.multiple_of(b * block, block), block)
        query = query_ref[at, :]
        tails = jnp.concatenate(tail_block(tail_ref, b, block), axis=1)
        pos = scale * jnp.sum(query * tails, axis=1, keepdims=True)
        neg = scale * lax.dot_general(query.astype(BF16), neg_ref[...], (((1,), (1,)), ((), ())), preferred_element_type=F32)
        top = jnp.maximum(pos, jnp.max(neg, axis=1, keepdims=True))
        pos_exp = jnp.exp(pos - top)
        neg_exp = jnp.exp(neg - top)
        denom = pos_exp + jnp.sum(neg_exp, axis=1, keepdims=True)
        weight = weight_ref[at, step_no:step_no + 1]
        loss = loss + weight * (top + jnp.log(denom) - pos)
        d_pos = weight * (pos_exp / denom - 1.0)
        d_neg = ((weight / denom) * neg_exp).astype(BF16)
        query_ref[at, :] = scale * (d_pos * tails + jnp.dot(d_neg, neg_ref[...], preferred_element_type=F32))
        return loss

    loss = lax.fori_loop(0, edges // block, body, jnp.zeros((block, 1), F32))
    tab_ref[areas['loss'][0] + step_no] = jnp.broadcast_to(jnp.sum(loss, axis=0, keepdims=True), (4, LANES))
    hold2, grad2 = flat(hold_ref), flat(grad_out)
    half = edges // 2
    step = half // 8
    for side, head_ref in enumerate((one_ref, two_ref)):
        for g in range(8):
            at = side * half + g * step
            heads = unpack_part(head_ref, half, g, step)
            rels = [plane(hold2, at, step, part) for part in range(4)]
            rels[3] = keep_data(rels[3])
            d_query = [query_ref[at:at + step, part * LANES:(part + 1) * LANES] for part in range(4)]
            d_head = times_conj(d_query, rels)
            d_rel = times_conj(d_query, heads)
            for part in range(4):
                put_plane(grad2, at, step, part, d_head[part])
                put_plane(hold2, at, step, part, d_rel[part])

    rel_rows = rel_tab.shape[0]
    sum_ref = grad_out.at[pl.ds(2 * edges, rel_rows)]
    sum_ref[...] = jnp.zeros(sum_ref.shape, F32)

    def scatter(b, acc):
        at = b * STEP
        grads = [hold_ref[plan_ref[at + u]] for u in range(STEP)]
        acc, sums = run_sums(acc, grads, [same_ref[at + u] for u in range(STEP)])
        for u in range(STEP):
            sum_ref[plan_ref[at + (edges + u)]] = sums[u]
        return acc

    lax.fori_loop(0, edges // STEP, scatter, jnp.zeros((4, LANES), F32))
    drel_out = flat(tab_ref.at[pl.ds(*areas['drel'])])
    pack_rows(drel_out, flat(sum_ref), rel_rows, 0, 8, None)
    used, half = rel_rows * 25 // 8, give_out.shape[0]
    drel_out[used:, :] = jnp.zeros((2 * half - used, LANES), F32)
    core = lax.rem(lax.axis_index('ent'), 2)
    give_out[...] = drel_out[pl.ds(pl.multiple_of((1 - core) * half, 8), half), :]


def tail_kernel(rel_ref, weight_ref, head_ref, tail_ref, tab_ref, query_ref, neg_ref, sum_ref, *, areas, side, last):
    rel_tab, grad_out = tab_ref.at[pl.ds(*areas['rel'])], tab_ref.at[pl.ds(*areas['grad'])]
    edges = neg_ref.shape[0]
    half = edges // 2
    hold_ref = grad_out.at[pl.ds(edges + side * half, half)]
    unpack_negs(tail_ref, neg_ref)

    copy_rows(rel_ref, half, rel_tab, hold_ref, side * half)
    put_queries(head_ref, flat(hold_ref), query_ref, 0)
    scale = DIM ** -0.5
    block = edges // 4
    grad2 = flat(grad_out)
    sum_ref[...] = jnp.zeros(sum_ref.shape, F32)

    def body(b, carry):
        at = pl.ds(pl.multiple_of(b * block, block), block)
        query = query_ref[at, :]
        query_bf = query.astype(BF16)
        tails = tail_block(tail_ref, b + 2 * side, block)
        prod = [query[:, part * LANES:(part + 1) * LANES] * tails[part] for part in range(4)]
        prod = (prod[0] + prod[1]) + (prod[2] + prod[3])
        pos = scale * jnp.sum(prod.T, axis=0, keepdims=True)
        neg = scale * lax.dot_general(neg_ref[...], query_bf, (((1,), (1,)), ((), ())), preferred_element_type=F32)
        top = jnp.maximum(pos, jnp.max(neg, axis=0, keepdims=True))
        pos_exp = jnp.exp(pos - top)
        neg_exp = jnp.exp(neg - top)
        denom = pos_exp + jnp.sum(neg_exp, axis=0, keepdims=True)
        weight = weight_ref[pl.ds(b + 2 * side, 1), :]
        d_pos = weight * (pos_exp / denom - 1.0)
        d_neg = ((weight / denom) * neg_exp).astype(BF16)
        sum_ref[...] += jnp.dot(d_neg, query_bf, preferred_element_type=F32)
        d_pos_col = jnp.broadcast_to(d_pos, (LANES, block)).T
        for part in range(4):
            grad2[pl.ds((edges + side * half + b * block) * 4 + part, block, stride=4), :] = scale * d_pos_col * query[:, part * LANES:(part + 1) * LANES]
        return carry

    lax.fori_loop(0, half // block, body, 0)
    for part in range(4):
        total = scale * sum_ref[:, part * LANES:(part + 1) * LANES]
        if last:
            total = total + plane(grad2, 2 * edges, edges, part)
        put_plane(grad2, 2 * edges, edges, part, total)


def split_kernel(got_ref, own_out, one_out, two_out, three_out, tab_ref, *, areas):
    drel_ref = flat(tab_ref.at[pl.ds(*areas['drel'])])
    half, piece = got_ref.shape[0], own_out.shape[0]
    me = lax.axis_index('ent')
    core, chip = lax.rem(me, 2), lax.div(me, 2)
    for away, out in enumerate((own_out, one_out, two_out, three_out)):
        at = pl.multiple_of((chip ^ away) * piece, 8)
        out[...] = drel_ref[pl.ds(pl.multiple_of(core * half + at, 8), piece), :] + got_ref[pl.ds(at, piece), :]


def sum_kernel(own_ref, one_ref, two_ref, three_ref, out, tab_ref, *, areas):
    out[...] = (own_ref[...] + one_ref[...]) + (two_ref[...] + three_ref[...])


def join_kernel(own_ref, one_ref, two_ref, three_ref, out, tab_ref, *, areas):
    piece = own_ref.shape[0]
    chip = lax.div(lax.axis_index('ent'), 2)
    for away, ref in enumerate((own_ref, one_ref, two_ref, three_ref)):
        out[pl.ds(pl.multiple_of((chip ^ away) * piece, 8), piece), :] = ref[...]


def rel_kernel(half_ref, far_ref, tab_ref, *, areas):
    drel_ref = flat(tab_ref.at[pl.ds(*areas['drel'])])
    rel_tab = tab_ref.at[pl.ds(*areas['rel'])]
    rows = rel_tab.shape[0]
    half = half_ref.shape[0]
    core = lax.rem(lax.axis_index('ent'), 2)
    drel_ref[pl.ds(pl.multiple_of(core * half, 8), half), :] = half_ref[...]
    drel_ref[pl.ds(pl.multiple_of((1 - core) * half, 8), half), :] = far_ref[...]
    step = rows // 8
    rel2 = flat(rel_tab)
    for g in range(8):
        grad = unpack_part(drel_ref, rows, g, step)
        row = [plane(rel2, g * step, step, part) for part in range(4)]
        new = adagrad(grad, row)
        for part in range(4):
            put_plane(rel2, g * step, step, part, new[part])


def shape(*dims, dtype=F32):
    return jax.ShapeDtypeStruct(dims, dtype)


def solution(mesh):
    ent_devs = mesh.shape['ent']
    row_spec = P(('sweep', 'ent'), None)
    state_spec = P(('sweep', 'ent'))
    rel_spec = P('sweep', None)
    edge_spec = P(('sweep', 'ent'), None, None)

    def train(ent_part, ada_part, rel_table, head_idx, tail_idx, rel_idx, neg_idx, edge_mask):
        part_rows = ent_part.shape[0]
        rel_count = rel_table.shape[0]
        rounds = head_idx.shape[1]
        edges = head_idx.shape[2]
        rel_rows = -(-rel_count // 128) * 128
        piece = -(-(rel_rows * 25 // 8) // 64) * 8
        head_idx, tail_idx, rel_idx, neg_idx, edge_mask = (x[0] for x in (head_idx, tail_idx, rel_idx, neg_idx, edge_mask))


        def away(bits):
            return [(sender, sender ^ bits) for sender in range(ent_devs)]

        def ring(step):
            shift = step + 1
            to_owner = [(sender, (sender + shift) % ent_devs) for sender in range(ent_devs)]
            return to_owner, [(target, sender) for sender, target in to_owner]

        asked = jnp.stack([tail_idx, neg_idx, rel_idx, edge_mask], axis=1)
        served = jnp.stack([lax.ppermute(asked[step], 'ent', ring(step)[0]) for step in range(rounds)])
        rows_all = jnp.concatenate([head_idx, served[:, 0], served[:, 1]], axis=1)
        keys = lax.sort(rows_all * 4096 + jnp.arange(3 * edges, dtype=jnp.int32)[None, :], dimension=1, is_stable=False)
        rel_keys = lax.sort(rel_idx * 1024 + jnp.arange(edges, dtype=jnp.int32)[None, :], dimension=1, is_stable=False)
        own_weight = jnp.pad(edge_mask.astype(F32), ((0, 8 - rounds), (0, 0))).T
        serve_weight = served[:, 3].astype(F32).reshape(rounds, edges // 256, 256)

        def plan(keys, bits, spare):
            rows, places = keys >> bits, keys & ((1 << bits) - 1)
            equal = rows[:, 1:] == rows[:, :-1]
            no = jnp.zeros((rounds, 1), jnp.bool_)
            parts = [places, rows]
            if spare is not None:
                parts.append(jnp.where(jnp.concatenate([equal, no], axis=1), spare, rows))
            return jnp.concatenate(parts, axis=1), jnp.concatenate([no, equal], axis=1).astype(F32)

        total_rows = part_rows + 2 * edges + max(edges, rel_rows) + rel_rows + 2 * piece + rounds
        moves, same = plan(keys, 12, total_rows)
        rel_moves, rel_same = plan(rel_keys, 10, None)
        small = []
        for step in range(rounds):
            small.append((head_idx[step], served[step, 0], served[step, 1], served[step, 2], rel_idx[step], moves[step], same[step], rel_moves[step], rel_same[step], serve_weight[step]))
        small, own_weight, rel_cols, ent_cols, ada_row = lax.optimization_barrier((small, own_weight, rel_table.T, ent_part.T, ada_part.reshape(1, part_rows)))

        cols = 512
        grad_rows = 2 * edges + max(edges, rel_rows)
        areas = {'grad': (part_rows, grad_rows), 'rel': (part_rows + grad_rows, rel_rows), 'drel': (part_rows + grad_rows + rel_rows, 2 * piece)}
        areas['loss'] = (sum(areas['drel']), rounds)
        tab_shape = pltpu.VMEM((total_rows + 2, 4, LANES), F32)
        head_wire, tail_wire = shape(edges * 25 // 16, LANES), shape(2 * edges * 25 // 8, LANES, dtype=BF16)
        part_wire, half_wire = shape(piece, LANES), shape(4 * piece, LANES)
        hold = pltpu.VMEM((edges, 4, LANES), F32)
        work = [pltpu.VMEM((edges, 512), F32), pltpu.VMEM((edges, 512), BF16)]

        def call(kernel, tab, inputs, in_specs, out_shape, out_specs, scratch=(), **more):
            ins, outs = len(inputs), len(out_shape)

            def body(*refs):
                kernel(*refs[:ins], *refs[ins + 2:ins + 2 + outs], refs[ins + 1], *refs[ins + 2 + outs:], areas=areas, **more)

            got = pl.pallas_call(
                body, in_specs=in_specs + [VM], out_specs=[VM] + out_specs, out_shape=[tab_shape] + out_shape,
                input_output_aliases={ins: 0}, scratch_shapes=list(scratch), compiler_params=params(GRANT))(*inputs, tab)
            return got[0], got[1:]

        tab = pl.pallas_call(
            load_kernel, in_specs=[HBM], out_specs=VM, out_shape=tab_shape,
            scratch_shapes=[pltpu.VMEM((4, DIM, cols), F32), pltpu.SemaphoreType.DMA((4,))],
            compiler_params=params(GRANT), name="load")(ent_cols)
        tab, _ = call(load_rel_kernel, tab, [rel_cols, ada_row], [VM, VM], [], [])
        half = None
        for step in range(rounds):
            to_owner, to_asker = ring(step)
            head_ids, serve_tails, serve_negs, serve_rel, own_rel, move, equal, rel_move, rel_equal, weight = small[step]
            tab, (tails,) = call(gather_tails_kernel, tab, [serve_tails, serve_negs], [SM] * 2, [tail_wire], [VM], [hold])
            far_tails = lax.ppermute(tails, 'ent', to_asker)
            tab, heads = call(gather_heads_kernel, tab, [head_ids], [SM], [head_wire] * 2, [VM] * 2, [hold])
            if TAILS_FIRST[step % len(TAILS_FIRST)]:
                far_tails, *heads = lax.optimization_barrier((far_tails, *heads))
            far_heads = []
            for side in range(2):
                far_heads.append(lax.ppermute(heads[side], 'ent', to_owner))
            if step:
                tab, _ = call(rel_kernel, tab, [half, far_half], [VM] * 2, [], [])

            def tail_role(tab, side, last):
                return call(
                    tail_kernel, tab, [serve_rel, weight, far_heads[side], tails], [SM, VM, VM, VM], [], [],
                    [pltpu.VMEM((edges // 2, 512), F32), pltpu.VMEM((edges, 512), BF16), pltpu.VMEM((edges, 512), F32)], side=side, last=last)[0]

            tab, (give,) = call(
                head_kernel, tab, [own_rel, rel_move, rel_equal, own_weight, *heads, far_tails], [SM] * 3 + [VM] * 4,
                [half_wire], [VM], work, step_no=step)
            got = lax.ppermute(give, 'ent', away(1))
            tab, (own, *parts) = call(split_kernel, tab, [got], [VM], [part_wire] * 4, [VM] * 4)
            parts = [lax.ppermute(x, 'ent', away(2 * hop + 2)) for hop, x in enumerate(parts)]
            tab = tail_role(tab, 0, False)
            tab = tail_role(tab, 1, True)
            tab, (total,) = call(sum_kernel, tab, [own, *parts], [VM] * 4, [part_wire], [VM])
            totals = [lax.ppermute(total, 'ent', away(2 * hop + 2)) for hop in range(3)]
            tab, _ = call(update_kernel, tab, [move, equal], [SM] * 2, [], [], [hold, hold])
            tab, (half,) = call(join_kernel, tab, [total, *totals], [VM] * 4, [half_wire], [VM])
            far_half = lax.ppermute(half, 'ent', away(1))
        tab, _ = call(rel_kernel, tab, [half, far_half], [VM] * 2, [], [])

        ent_out, ada_out = pl.pallas_call(
            store_kernel, grid=(part_rows // cols,), in_specs=[VM],
            out_specs=[pl.BlockSpec((DIM, cols), lambda i: (0, i)), pl.BlockSpec((1, cols), lambda i: (0, i))],
            out_shape=[shape(DIM, part_rows), shape(1, part_rows)], compiler_params=params(GRANT), name="store")(tab)
        rel_out, loss_out = pl.pallas_call(
            functools.partial(store_rel_kernel, areas=areas, edges=edges), in_specs=[VM], out_specs=[VM, VM],
            out_shape=[shape(DIM, rel_count), shape(1, LANES)], compiler_params=params(GRANT), name="store_rel")(tab)
        ent_out, ada_out, rel_out, loss_out = lax.optimization_barrier((ent_out, ada_out, rel_out, loss_out))
        return ent_out.T, ada_out.reshape(part_rows), rel_out.T, loss_out[:, :rounds]

    return jax.shard_map(train, mesh=mesh, in_specs=(row_spec, state_spec, rel_spec, edge_spec, edge_spec, edge_spec, edge_spec, edge_spec), out_specs=(row_spec, state_spec, rel_spec, row_spec), check_vma=False)
```
